8 devices in a mesh: z: 2 (over z, y), y: 2 (over x), xc: 2 (over core).
Axes of the slice: x: 2, y: 2, z: 1, core: 2. Of those that a mesh axis runs over, the one named last changes fastest.
Arguments:
- tokens_x: bfloat16 [65536, 512], P(('z', 'y', 'xc'))
- grad_y: bfloat16 [65536, 512], P(('z', 'y', 'xc'))
- w_one: bfloat16 [512, 2048], replicated
- w_two: bfloat16 [2048, 512], replicated
- w_three: bfloat16 [512, 2048], replicated
- w_four: bfloat16 [2048, 512], replicated
Outputs:
- output 1: float32 [512, 2048], replicated
- output 2: float32 [2048, 512], replicated
- output 3: float32 [512, 2048], replicated
- output 4: float32 [2048, 512], replicated
All inputs are finite; a program needn't handle non-finite values.
Results may differ from the reference program's by a relative error of at most 0.00328.
Values are sent between devices in bfloat16 or wider.
A program may use at most 1 GiB of HBM per device.

```python
import math
import jax
import jax.numpy as jnp
from jax import lax

D = 512
FF = 2048
TOKENS_DEV = 8192
DEVICES = 8

TOKENS = DEVICES * TOKENS_DEV
GELU_SCALE = math.sqrt(2.0 / math.pi)
GELU_CUBIC = 0.044715


def gelu_value(pre_act):
    return 0.5 * pre_act * (1.0 + jnp.tanh(GELU_SCALE * (pre_act + GELU_CUBIC * pre_act * pre_act * pre_act)))


def gelu_grad(pre_act):
    tanh_val = jnp.tanh(GELU_SCALE * (pre_act + GELU_CUBIC * pre_act * pre_act * pre_act))
    return 0.5 * (1.0 + tanh_val) + 0.5 * pre_act * (1.0 - tanh_val * tanh_val) * GELU_SCALE * (1.0 + 3.0 * GELU_CUBIC * pre_act * pre_act)


def setup_inputs(seed: int = 0) -> dict:
    root_key = jax.random.key(seed)
    key_list = jax.random.split(root_key, 8)
    scale_x = jax.random.uniform(key_list[0], (DEVICES, 1, 1), jnp.float32, 0.7, 1.3)
    scale_g = jax.random.uniform(key_list[1], (DEVICES, 1, 1), jnp.float32, 0.7, 1.3)
    x_rows = jax.random.normal(key_list[2], (DEVICES, TOKENS_DEV, D), jnp.float32) * scale_x
    g_rows = jax.random.normal(key_list[3], (DEVICES, TOKENS_DEV, D), jnp.float32) * scale_g
    w_one = jax.random.normal(key_list[4], (D, FF), jnp.float32) * D ** -0.5
    w_two = jax.random.normal(key_list[5], (FF, D), jnp.float32) * FF ** -0.5
    w_three = jax.random.normal(key_list[6], (D, FF), jnp.float32) * D ** -0.5
    w_four = jax.random.normal(key_list[7], (FF, D), jnp.float32) * FF ** -0.5
    return {
        "tokens_x": x_rows.reshape(TOKENS, D).astype(jnp.bfloat16),
        "grad_y": g_rows.reshape(TOKENS, D).astype(jnp.bfloat16),
        "w_one": w_one.astype(jnp.bfloat16),
        "w_two": w_two.astype(jnp.bfloat16),
        "w_three": w_three.astype(jnp.bfloat16),
        "w_four": w_four.astype(jnp.bfloat16),
    }


def local_grads(x_loc, g_loc, w_one, w_two, w_three, w_four):
    a_one = jnp.dot(x_loc, w_one, preferred_element_type=jnp.float32).astype(jnp.bfloat16)
    h_one = gelu_value(a_one.astype(jnp.float32)).astype(jnp.bfloat16)
    h_two = (jnp.dot(h_one, w_two, preferred_element_type=jnp.float32) + x_loc.astype(jnp.float32)).astype(jnp.bfloat16)
    a_three = jnp.dot(h_two, w_three, preferred_element_type=jnp.float32).astype(jnp.bfloat16)
    h_three = gelu_value(a_three.astype(jnp.float32)).astype(jnp.bfloat16)
    d_w4 = jnp.dot(h_three.T, g_loc, preferred_element_type=jnp.float32)
    d_a3 = (jnp.dot(g_loc, w_four.T, preferred_element_type=jnp.float32) * gelu_grad(a_three.astype(jnp.float32))).astype(jnp.bfloat16)
    d_w3 = jnp.dot(h_two.T, d_a3, preferred_element_type=jnp.float32)
    d_h2 = (jnp.dot(d_a3, w_three.T, preferred_element_type=jnp.float32) + g_loc.astype(jnp.float32)).astype(jnp.bfloat16)
    d_w2 = jnp.dot(h_one.T, d_h2, preferred_element_type=jnp.float32)
    d_a1 = (jnp.dot(d_h2, w_two.T, preferred_element_type=jnp.float32) * gelu_grad(a_one.astype(jnp.float32))).astype(jnp.bfloat16)
    d_w1 = jnp.dot(x_loc.T, d_a1, preferred_element_type=jnp.float32)
    return d_w1, d_w2, d_w3, d_w4


def reference(tokens_x, grad_y, w_one, w_two, w_three, w_four):
    x_shards = tokens_x.reshape(DEVICES, TOKENS_DEV, D)
    g_shards = grad_y.reshape(DEVICES, TOKENS_DEV, D)

    def accumulate(running, pair):
        x_loc, g_loc = pair
        grads = local_grads(x_loc, g_loc, w_one, w_two, w_three, w_four)
        return tuple(acc + new for acc, new in zip(running, grads)), None

    start_sums = (
        jnp.zeros((D, FF), jnp.float32),
        jnp.zeros((FF, D), jnp.float32),
        jnp.zeros((D, FF), jnp.float32),
        jnp.zeros((FF, D), jnp.float32),
    )
    totals, _ = lax.scan(accumulate, start_sums, (x_shards, g_shards))
    return (totals[0] / DEVICES, totals[1] / DEVICES, totals[2] / DEVICES, totals[3] / DEVICES)
```

```python
import functools
import math

import jax
import jax.numpy as jnp
from jax import lax
from jax.experimental import pallas as pl
from jax.experimental.pallas import tpu as pltpu
from jax.sharding import PartitionSpec as P

MESH = pl.DeviceIdType.MESH
GELU_C = math.sqrt(2.0 / math.pi)
GELU_K = 0.044715

N = 8192
D = 512
F = 2048
FB = 256
NB = F // FB
T1 = 512
N1 = N // T1
T2 = 2048
N2 = N // T2
RC = 256
SLOTS = 4
OFFS = (0, 1, 4, 6, 8, 11, 13)
LAST_TRIP = 73 + OFFS[-1]

bf16 = jnp.bfloat16
f32 = jnp.float32


def dot(a, b):
    return jnp.dot(a, b, preferred_element_type=f32)


def dot_nt(a, b):
    return lax.dot_general(a, b, (((1,), (1,)), ((), ())), preferred_element_type=f32)


def gelu_half(a):
    sq = a * a
    t = jnp.tanh(a * (GELU_C + (GELU_C * GELU_K) * sq))
    s = 0.5 + 0.5 * t
    return sq, s, a * s


def gelu_and_grad(a):
    sq, s, h = gelu_half(a)
    g = s + (h * (1.0 - s)) * (2.0 * GELU_C + (6.0 * GELU_C * GELU_K) * sq)
    return h, g


def kernel(x_hbm, g_hbm, w1_hbm, w2_hbm, w3_hbm, w4_hbm, out, a1_hbm, da3_hbm,
           gn, gt, hn, ht, w1, w2, w3, w4, u0, u1, u2, u3, vv, xs,
           pacc, rx, sm, r1, r2, rs,
           ld_sem, x_sem, st_sem, ld2_sem, send_sem, recv_sem, loc_sem):
    z = lax.axis_index("z")
    y = lax.axis_index("y")
    c = lax.axis_index("xc")
    partner = (z, y, 1 - c)
    near_a = (lax.rem(z + c, 2), lax.rem(y + 1 - c, 2), c)
    near_b = (lax.rem(z + 1 - c, 2), lax.rem(y + c, 2), c)
    bit_a = y * (1 - c) + z * c
    bit_b = z * (1 - c) + y * c

    barrier = pltpu.get_barrier_semaphore()
    for dev in (partner, near_a, near_b):
        pl.semaphore_signal(barrier, inc=1, device_id=dev, device_id_type=MESH)

    def x_copy(i):
        slot = lax.rem(i, 4)
        return pltpu.make_async_copy(x_hbm.at[pl.ds(i * T1, T1)], xs.at[slot], x_sem.at[slot])

    loads = [
        pltpu.make_async_copy(w1_hbm, w1, ld_sem.at[0]),
        pltpu.make_async_copy(w2_hbm, w2, ld_sem.at[1]),
        pltpu.make_async_copy(g_hbm, gn, ld_sem.at[2]),
        pltpu.make_async_copy(w3_hbm, w3, ld_sem.at[3]),
        pltpu.make_async_copy(w4_hbm, w4, ld_sem.at[4]),
    ]
    loads[0].start()
    x_copy(0).start()
    x_copy(1).start()
    for ld in loads[1:]:
        ld.start()
    pl.semaphore_wait(barrier, 3)

    uu = (u0, u1, u2, u3)

    def a1_store(i, par, cc):
        return pltpu.make_async_copy(
            vv.at[2 * par + cc // 4, pl.ds((cc % 4) * T1, T1)],
            a1_hbm.at[cc, pl.ds(i * T1, T1)],
            st_sem.at[par],
        )

    def fwd_trip(i, par, wait_x):
        prev = lax.rem(i + N1 - 1, N1)
        if wait_x:
            x_copy(i).wait()
        xt = xs.at[lax.rem(i, 4)]
        acc = xs[lax.rem(i + 3, 4)].astype(f32)
        for cc in range(NB):
            a = dot(xt[...], w1[:, cc * FB:(cc + 1) * FB]).astype(bf16)
            vv[2 * par + cc // 4, (cc % 4) * T1:(cc % 4 + 1) * T1, :] = a
            _, _, h = gelu_half(a.astype(f32))
            uu[2 * par + cc // 4][(cc % 4) * T1:(cc % 4 + 1) * T1, :] = h.astype(bf16)
        res = None
        for cc in range(NB):
            hb = uu[2 * (1 - par) + cc // 4][(cc % 4) * T1:(cc % 4 + 1) * T1, :]
            term = dot(hb, w2[cc * FB:(cc + 1) * FB, :])
            res = term if res is None else res + term
        h2 = (res + acc).astype(bf16)
        hn[pl.ds(pl.multiple_of(prev * T1, T1), T1), :] = h2
        ht[prev // 4, :, pl.ds(pl.multiple_of(lax.rem(prev, 4) * T1, T1), T1)] = h2.T
        gt[i // 4, :, pl.ds(pl.multiple_of(lax.rem(i, 4) * T1, T1), T1)] = gn[pl.ds(pl.multiple_of(i * T1, T1), T1), :].T

    for ld in loads[:3]:
        ld.wait()

    def fwd_pair(k, carry):
        for par in (0, 1):
            i = 2 * k + par

            @pl.when(i >= 2)
            def _():
                for cc in range(NB):
                    a1_store(i - 2, par, cc).wait()

            @pl.when(i + 2 < N1)
            def _():
                x_copy(i + 2).start()

            x_copy(i).wait()
            fwd_trip(i, par, False)
            for cc in range(NB):
                a1_store(i, par, cc).start()
        return carry

    lax.fori_loop(0, N1 // 2, fwd_pair, 0)
    res = None
    for cc in range(NB):
        hb = uu[2 + cc // 4][(cc % 4) * T1:(cc % 4 + 1) * T1, :]
        term = dot(hb, w2[cc * FB:(cc + 1) * FB, :])
        res = term if res is None else res + term
    h2 = (res + xs[(N1 - 1) % 4].astype(f32)).astype(bf16)
    hn[N - T1:N, :] = h2
    ht[N2 - 1, :, T2 - T1:T2] = h2.T
    for par in (0, 1):
        for cc in range(NB):
            a1_store(N1 - 2 + par, par, cc).wait()
    for ld in loads[3:]:
        ld.wait()

    def half(b):
        return pl.ds(pl.multiple_of(b * (D // 2), D // 2), D // 2)

    def quarter(a, b):
        return pl.ds(pl.multiple_of(a * (D // 2) + b * (D // 4), D // 4), D // 4)

    def remote(src, dst, slot, step, dev):
        return pltpu.make_async_remote_copy(
            src_ref=src, dst_ref=dst, send_sem=send_sem.at[slot, step], recv_sem=recv_sem.at[slot, step],
            device_id=dev, device_id_type=MESH)

    def cp_pair(p, s):
        return remote(pacc.at[lax.rem(p, 2), 1 - c], rx.at[s], s, 0, partner)

    def cp_s1(p, s):
        return remote(sm.at[s, half(1 - bit_a)], r1.at[s], s, 1, near_a)

    def cp_s2(p, s):
        return remote(sm.at[s, quarter(bit_a, 1 - bit_b)], r2.at[s], s, 2, near_b)

    def cp_s3(p, s):
        rows = quarter(bit_a, bit_b)
        return remote(rs.at[s, rows], rs.at[s, rows], s, 3, near_b)

    def cp_s4(p, s):
        rows = half(bit_a)
        return remote(rs.at[s, rows], rs.at[s, rows], s, 4, near_a)

    def cp_s5(p, s):
        return remote(rs.at[s], out.at[p, c], s, 5, partner)

    def cp_loc(p, s):
        return pltpu.make_async_copy(rs.at[s], out.at[p, c], loc_sem.at[s])

    def h_pair_send(p, s):
        cp_pair(p, s).start()

    def h_s1(p, s):
        cp_pair(p, s).wait()
        sm[s] = pacc[lax.rem(p, 2), c] + rx[s]
        cp_s1(p, s).start()

    def h_s2(p, s):
        cp_s1(p, s).wait()
        rows = half(bit_a)
        sm[s, rows] = sm[s, rows] + r1[s]
        cp_s2(p, s).start()

    def h_s3(p, s):
        cp_s2(p, s).wait()
        rows = quarter(bit_a, bit_b)
        rs[s, rows] = (sm[s, rows] + r2[s]) * 0.125
        cp_s3(p, s).start()

    def h_s4(p, s):
        cp_s3(p, s).wait()
        cp_s4(p, s).start()

    def h_s5(p, s):
        cp_s4(p, s).wait()
        cp_s5(p, s).start()
        cp_loc(p, s).start()

    def h_end(p, s):
        cp_s5(p, s).wait()
        cp_loc(p, s).wait()

    stages = (h_pair_send, h_s1, h_s2, h_s3, h_s4, h_s5, h_end)

    def comm(f):
        for order in (0, 6, 5, 4, 3, 2, 1):
            q = f + (40 - 5 - OFFS[order])
            k = q // 4 - 10
            ok = jnp.logical_and(
                lax.rem(q, 4) == 0,
                jnp.logical_or(jnp.logical_and(k >= 0, k < NB), jnp.logical_and(k >= NB + 2, k < 2 * NB + 2)))

            @pl.when(ok)
            def _():
                p = jnp.where(k >= NB + 2, k - 2, k)
                stages[order](p, lax.rem(p, SLOTS))

    def accumulate(par, idx, first, value):
        old = pacc[par, idx]
        if first is not None:
            old = jnp.where(first, 0.0, old)
        pacc[par, idx] = old + value

    def b_part(lhs0, lhs1, tb, par, pb, first):
        accumulate(par, 0, first, dot(lhs0[tb], uu[pb][...]))
        accumulate(par, 1, first, dot(lhs1[tb], uu[2 + pb][...]))

    def da3_store(f, par):
        return pltpu.make_async_copy(
            uu[2 + par], da3_hbm.at[f // N2, pl.ds(lax.rem(f, N2) * T2, T2)], st_sem.at[par])

    def l2_trip(f, par):
        t = lax.rem(f, N2)
        j = f // N2
        col = pl.ds(pl.multiple_of(j * FB, FB), FB)
        before = f + N2 - 1
        tb = lax.rem(before, N2)
        pp = lax.rem(before // N2 + 1, 2)
        w3j = w3[:, col]
        w4j = w4[col, :]
        for rc in range(T2 // RC):
            rows = pl.ds(pl.multiple_of(t * T2 + rc * RC, RC), RC)
            a = dot(hn[rows, :], w3j).astype(bf16).astype(f32)
            d = dot_nt(gn[rows, :], w4j)
            h, g = gelu_and_grad(a)
            uu[par][rc * RC:(rc + 1) * RC, :] = h.astype(bf16)
            uu[2 + par][rc * RC:(rc + 1) * RC, :] = (d * g).astype(bf16)
        b_part(gt, ht, tb, pp, 1 - par, None if par == 0 else tb == 0)

    def l2_pair(k, carry):
        for par in (0, 1):
            f = 2 * k + par
            comm(f)

            @pl.when(f >= 2)
            def _():
                da3_store(f - 2, par).wait()

            l2_trip(f, par)
            da3_store(f, par).start()
        return carry

    lax.fori_loop(0, NB * N2 // 2, l2_pair, 0)
    b_part(gt, ht, N2 - 1, (NB - 1) % 2, 1, None)
    for par in (0, 1):
        da3_store(NB * N2 - 2 + par, par).wait()

    def da3_load(i, par, cc):
        return pltpu.make_async_copy(
            da3_hbm.at[cc, pl.ds(i * T1, T1)],
            vv.at[2 * par + cc // 4, pl.ds((cc % 4) * T1, T1)],
            ld2_sem.at[par],
        )

    def da3_start(i, par):
        for cc in range(NB):
            da3_load(i, par, cc).start()
        x_copy(i).start()

    da3_start(0, 0)
    da3_start(1, 1)

    def dh2_pair(k, carry):
        comm(NB * N2 + k)
        for par in (0, 1):
            i = 2 * k + par
            for cc in range(NB):
                da3_load(i, par, cc).wait()
            x_copy(i).wait()
            rows = pl.ds(pl.multiple_of(i * T1, T1), T1)
            lanes = pl.ds(pl.multiple_of(lax.rem(i, 4) * T1, T1), T1)
            res = None
            for cc in range(NB):
                term = dot_nt(vv[2 * par + cc // 4, (cc % 4) * T1:(cc % 4 + 1) * T1, :], w3[:, cc * FB:(cc + 1) * FB])
                res = term if res is None else res + term
            dh2 = (res + gn[rows, :].astype(f32)).astype(bf16)
            hn[rows, :] = dh2
            ht[i // 4, :, lanes] = dh2.T
            gt[i // 4, :, lanes] = xs[lax.rem(i, 4)].T

            @pl.when(i + 2 < N1)
            def _():
                da3_start(i + 2, par)
        return carry

    lax.fori_loop(0, N1 // 2, dh2_pair, 0)

    base = NB * N2 + N1 // 2

    def a1_load(f):
        slot = lax.rem(f, 4)
        return pltpu.make_async_copy(
            a1_hbm.at[f // N2, pl.ds(lax.rem(f, N2) * T2, T2)], vv.at[slot], x_sem.at[slot])

    for f0 in range(3):
        a1_load(f0).start()

    def l1_trip(f, par):
        t = lax.rem(f, N2)
        j = f // N2
        col = pl.ds(pl.multiple_of(j * FB, FB), FB)
        before = f + N2 - 1
        tb = lax.rem(before, N2)
        pp = lax.rem(before // N2 + 1, 2)
        slot = lax.rem(f, 4)
        w2j = w2[col, :]
        for rc in range(T2 // RC):
            rows = pl.ds(pl.multiple_of(t * T2 + rc * RC, RC), RC)
            a = vv[slot, rc * RC:(rc + 1) * RC, :].astype(f32)
            d = dot_nt(hn[rows, :], w2j)
            h, g = gelu_and_grad(a)
            uu[par][rc * RC:(rc + 1) * RC, :] = h.astype(bf16)
            uu[2 + par][rc * RC:(rc + 1) * RC, :] = (d * g).astype(bf16)
        b_part(ht, gt, tb, pp, 1 - par, None if par == 0 else tb == 0)

    def l1_pair(k, carry):
        for par in (0, 1):
            f = 2 * k + par
            comm(base + f)

            @pl.when(f + 3 < NB * N2)
            def _():
                a1_load(f + 3).start()

            a1_load(f).wait()
            l1_trip(f, par)
        return carry

    lax.fori_loop(0, NB * N2 // 2, l1_pair, 0)
    comm(base + NB * N2)
    b_part(ht, gt, N2 - 1, (NB - 1) % 2, 1, None)

    def tail(k, carry):
        comm(base + NB * N2 + 1 + k)
        return carry

    lax.fori_loop(0, LAST_TRIP - base - NB * N2, tail, 0)


def finish_kernel(p2, p1, o1, o2, o3, o4):
    o1[...] = p1[0, 1]
    o2[...] = p1[0, 0].T
    o3[...] = p2[0, 1]
    o4[...] = p2[0, 0].T


def device_step(x_loc, g_loc, w_one, w_two, w_three, w_four):
    any_spec = pl.BlockSpec(memory_space=pl.ANY)
    sums, _, _ = pl.pallas_call(
        kernel,
        name="grads",
        out_shape=(
            jax.ShapeDtypeStruct((2 * NB, 2, D, FB), f32),
            jax.ShapeDtypeStruct((NB, N, FB), bf16),
            jax.ShapeDtypeStruct((NB, N, FB), bf16),
        ),
        in_specs=[any_spec] * 6,
        out_specs=(any_spec,) * 3,
        scratch_shapes=[
            pltpu.VMEM((N, D), bf16),
            pltpu.VMEM((N2, D, T2), bf16),
            pltpu.VMEM((N, D), bf16),
            pltpu.VMEM((N2, D, T2), bf16),
            pltpu.VMEM((D, F), bf16),
            pltpu.VMEM((F, D), bf16),
            pltpu.VMEM((D, F), bf16),
            pltpu.VMEM((F, D), bf16),
            pltpu.VMEM((T2, FB), bf16),
            pltpu.VMEM((T2, FB), bf16),
            pltpu.VMEM((T2, FB), bf16),
            pltpu.VMEM((T2, FB), bf16),
            pltpu.VMEM((4, T2, FB), bf16),
            pltpu.VMEM((4, T1, D), bf16),
            pltpu.VMEM((2, 2, D, FB), f32),
            pltpu.VMEM((SLOTS, D, FB), f32),
            pltpu.VMEM((SLOTS, D, FB), f32),
            pltpu.VMEM((SLOTS, D // 2, FB), f32),
            pltpu.VMEM((SLOTS, D // 4, FB), f32),
            pltpu.VMEM((SLOTS, D, FB), f32),
            pltpu.SemaphoreType.DMA((5,)),
            pltpu.SemaphoreType.DMA((4,)),
            pltpu.SemaphoreType.DMA((2,)),
            pltpu.SemaphoreType.DMA((2,)),
            pltpu.SemaphoreType.DMA((SLOTS, 6)),
            pltpu.SemaphoreType.DMA((SLOTS, 6)),
            pltpu.SemaphoreType.DMA((SLOTS,)),
        ],
        compiler_params=pltpu.CompilerParams(
            collective_id=0, has_side_effects=True, vmem_limit_bytes=67000000),
        cost_estimate=pl.CostEstimate(flops=20 * N * D * F, bytes_accessed=200 << 20, transcendentals=3 * N * F),
    )(x_loc, g_loc, w_one, w_two, w_three, w_four)
    wide = jax.ShapeDtypeStruct((D, F), f32)
    tall = jax.ShapeDtypeStruct((F, D), f32)
    wide_spec = pl.BlockSpec((D, FB), lambda j: (0, j))
    tall_spec = pl.BlockSpec((FB, D), lambda j: (j, 0))
    return pl.pallas_call(
        finish_kernel,
        name="finish",
        grid=(NB,),
        out_shape=(wide, tall, wide, tall),
        in_specs=[
            pl.BlockSpec((1, 2, D, FB), lambda j: (j, 0, 0, 0)),
            pl.BlockSpec((1, 2, D, FB), lambda j: (j + NB, 0, 0, 0)),
        ],
        out_specs=(wide_spec, tall_spec, wide_spec, tall_spec),
    )(sums, sums)


def solution(mesh):
    batch_spec = P(("z", "y", "xc"), None)
    whole_spec = P(None, None)
    return jax.shard_map(
        device_step,
        mesh=mesh,
        in_specs=(batch_spec, batch_spec, whole_spec, whole_spec, whole_spec, whole_spec),
        out_specs=(whole_spec, whole_spec, whole_spec, whole_spec),
        check_vma=False,
    )
```

```python
import functools
import math

import jax
import jax.numpy as jnp
from jax import lax
from jax.experimental import pallas as pl
from jax.experimental.pallas import tpu as pltpu
from jax.sharding import PartitionSpec as P

MESH = pl.DeviceIdType.MESH
GELU_C = math.sqrt(2.0 / math.pi)
GELU_K = 0.044715

N = 8192
D = 512
F = 2048
FB = 256
NB = F // FB
T1 = 512
N1 = N // T1
T2 = 2048
N2 = N // T2
RC = 256
SLOTS = 4
SEMS = 8
OFFS = (0, 2, 6, 9, 12, 16, 18)
LAST_TRIP = 73 + OFFS[-1]

bf16 = jnp.bfloat16
f32 = jnp.float32


def dot(a, b):
    return jnp.dot(a, b, preferred_element_type=f32)


def dot_nt(a, b):
    return lax.dot_general(a, b, (((1,), (1,)), ((), ())), preferred_element_type=f32)


def gelu_half(a):
    sq = a * a
    t = jnp.tanh(a * (GELU_C + (GELU_C * GELU_K) * sq))
    s = 0.5 + 0.5 * t
    return sq, s, a * s


def gelu_and_grad(a):
    sq, s, h = gelu_half(a)
    g = s + (h * (1.0 - s)) * (2.0 * GELU_C + (6.0 * GELU_C * GELU_K) * sq)
    return h, g


def kernel(x_hbm, g_hbm, w1_hbm, w2_hbm, w3_hbm, w4_hbm, out, a1_hbm, da3_hbm,
           gn, gt, hn, ht, w1, w2, w3, w4, u0, u1, u2, u3, vv, xs,
           pacc, rx, sm, r1, r2, rs,
           ld_sem, x_sem, st_sem, ld2_sem, send_sem, recv_sem, loc_sem):
    z = lax.axis_index("z")
    y = lax.axis_index("y")
    c = lax.axis_index("xc")
    partner = (z, y, 1 - c)
    near_a = (lax.rem(z + c, 2), lax.rem(y + 1 - c, 2), c)
    near_b = (lax.rem(z + 1 - c, 2), lax.rem(y + c, 2), c)
    bit_a = y * (1 - c) + z * c
    bit_b = z * (1 - c) + y * c

    barrier = pltpu.get_barrier_semaphore()
    for dev in (partner, near_a, near_b):
        pl.semaphore_signal(barrier, inc=1, device_id=dev, device_id_type=MESH)

    def x_copy(i):
        slot = lax.rem(i, 4)
        return pltpu.make_async_copy(x_hbm.at[pl.ds(i * T1, T1)], xs.at[slot], x_sem.at[slot])

    loads = [
        pltpu.make_async_copy(w1_hbm, w1, ld_sem.at[0]),
        pltpu.make_async_copy(w2_hbm, w2, ld_sem.at[1]),
        pltpu.make_async_copy(g_hbm, gn, ld_sem.at[2]),
        pltpu.make_async_copy(w3_hbm, w3, ld_sem.at[3]),
        pltpu.make_async_copy(w4_hbm, w4, ld_sem.at[4]),
    ]
    loads[0].start()
    x_copy(0).start()
    x_copy(1).start()
    for ld in loads[1:]:
        ld.start()
    pl.semaphore_wait(barrier, 3)

    uu = (u0, u1, u2, u3)

    def a1_store(i, par, cc):
        return pltpu.make_async_copy(
            vv.at[2 * par + cc // 4, pl.ds((cc % 4) * T1, T1)],
            a1_hbm.at[cc, pl.ds(i * T1, T1)],
            st_sem.at[par],
        )

    def fwd_trip(i, par, wait_x):
        prev = lax.rem(i + N1 - 1, N1)
        if wait_x:
            x_copy(i).wait()
        xt = xs.at[lax.rem(i, 4)]
        acc = xs[lax.rem(i + 3, 4)].astype(f32)
        for cc in range(NB):
            a = dot(xt[...], w1[:, cc * FB:(cc + 1) * FB]).astype(bf16)
            vv[2 * par + cc // 4, (cc % 4) * T1:(cc % 4 + 1) * T1, :] = a
            _, _, h = gelu_half(a.astype(f32))
            uu[2 * par + cc // 4][(cc % 4) * T1:(cc % 4 + 1) * T1, :] = h.astype(bf16)
        res = None
        for cc in range(NB):
            hb = uu[2 * (1 - par) + cc // 4][(cc % 4) * T1:(cc % 4 + 1) * T1, :]
            term = dot(hb, w2[cc * FB:(cc + 1) * FB, :])
            res = term if res is None else res + term
        h2 = (res + acc).astype(bf16)
        hn[pl.ds(pl.multiple_of(prev * T1, T1), T1), :] = h2
        ht[prev // 4, :, pl.ds(pl.multiple_of(lax.rem(prev, 4) * T1, T1), T1)] = h2.T
        gt[i // 4, :, pl.ds(pl.multiple_of(lax.rem(i, 4) * T1, T1), T1)] = gn[pl.ds(pl.multiple_of(i * T1, T1), T1), :].T

    for ld in loads[:3]:
        ld.wait()

    def fwd_pair(k, carry):
        for par in (0, 1):
            i = 2 * k + par

            @pl.when(i >= 2)
            def _():
                for cc in range(NB):
                    a1_store(i - 2, par, cc).wait()

            @pl.when(i + 2 < N1)
            def _():
                x_copy(i + 2).start()

            x_copy(i).wait()
            fwd_trip(i, par, False)
            for cc in range(NB):
                a1_store(i, par, cc).start()
        return carry

    lax.fori_loop(0, N1 // 2, fwd_pair, 0)
    res = None
    for cc in range(NB):
        hb = uu[2 + cc // 4][(cc % 4) * T1:(cc % 4 + 1) * T1, :]
        term = dot(hb, w2[cc * FB:(cc + 1) * FB, :])
        res = term if res is None else res + term
    h2 = (res + xs[(N1 - 1) % 4].astype(f32)).astype(bf16)
    hn[N - T1:N, :] = h2
    ht[N2 - 1, :, T2 - T1:T2] = h2.T
    for par in (0, 1):
        for cc in range(NB):
            a1_store(N1 - 2 + par, par, cc).wait()
    for ld in loads[3:]:
        ld.wait()

    def half(b):
        return pl.ds(pl.multiple_of(b * (D // 2), D // 2), D // 2)

    def quarter(a, b):
        return pl.ds(pl.multiple_of(a * (D // 2) + b * (D // 4), D // 4), D // 4)

    def remote(src, dst, p, step, dev):
        e = lax.rem(p, SEMS)
        return pltpu.make_async_remote_copy(
            src_ref=src, dst_ref=dst, send_sem=send_sem.at[e, step], recv_sem=recv_sem.at[e, step],
            device_id=dev, device_id_type=MESH)

    def cp_pair(p):
        e = lax.rem(p, 2)
        return remote(pacc.at[e, 1 - c], rx.at[e], p, 0, partner)

    def cp_s1(p):
        e = lax.rem(p, 2)
        return remote(sm.at[e, half(1 - bit_a)], r1.at[e], p, 1, near_a)

    def cp_s2(p):
        e = lax.rem(p, 2)
        return remote(sm.at[e, quarter(bit_a, 1 - bit_b)], r2.at[e], p, 2, near_b)

    def cp_s3(p):
        part = rs.at[lax.rem(p, SLOTS), quarter(bit_a, bit_b)]
        return remote(part, part, p, 3, near_b)

    def cp_s4(p):
        part = rs.at[lax.rem(p, SLOTS), half(bit_a)]
        return remote(part, part, p, 4, near_a)

    def cp_s5(p):
        return remote(rs.at[lax.rem(p, SLOTS)], out.at[p, c], p, 5, partner)

    def cp_loc(p):
        e = lax.rem(p, SLOTS)
        return pltpu.make_async_copy(rs.at[e], out.at[p, c], loc_sem.at[e])

    def h_pair_send(p):
        cp_pair(p).start()

    def h_s1(p):
        cp_pair(p).wait()
        e = lax.rem(p, 2)
        sm[e] = pacc[e, c] + rx[e]
        cp_s1(p).start()

    def h_s2(p):
        cp_s1(p).wait()
        e = lax.rem(p, 2)
        rows = half(bit_a)
        sm[e, rows] = sm[e, rows] + r1[e]
        cp_s2(p).start()

    def h_s3(p):
        cp_s2(p).wait()
        e = lax.rem(p, 2)
        rows = quarter(bit_a, bit_b)
        rs[lax.rem(p, SLOTS), rows] = (sm[e, rows] + r2[e]) * 0.125
        cp_s3(p).start()

    def h_s4(p):
        cp_s3(p).wait()
        cp_s4(p).start()

    def h_s5(p):
        cp_s4(p).wait()
        cp_s5(p).start()
        cp_loc(p).start()

    def h_end(p):
        cp_s5(p).wait()
        cp_loc(p).wait()

    stages = (h_pair_send, h_s1, h_s2, h_s3, h_s4, h_s5, h_end)

    def comm(f):
        for order in (0, 6, 5, 4, 3, 2, 1):
            q = f + (40 - 5 - OFFS[order])
            k = q // 4 - 10
            ok = jnp.logical_and(
                lax.rem(q, 4) == 0,
                jnp.logical_or(jnp.logical_and(k >= 0, k < NB), jnp.logical_and(k >= NB + 2, k < 2 * NB + 2)))

            @pl.when(ok)
            def _():
                stages[order](k - 2 * (k // (NB + 2)))

    def accumulate(par, idx, first, value):
        old = pacc[par, idx]
        if first is not None:
            old = jnp.where(first, 0.0, old)
        pacc[par, idx] = old + value

    def b_part(lhs0, lhs1, tb, par, pb, first):
        accumulate(par, 0, first, dot(lhs0[tb], uu[pb][...]))
        accumulate(par, 1, first, dot(lhs1[tb], uu[2 + pb][...]))

    def da3_store(f, par):
        return pltpu.make_async_copy(
            uu[2 + par], da3_hbm.at[f // N2, pl.ds(lax.rem(f, N2) * T2, T2)], st_sem.at[par])

    def l2_trip(f, par):
        t = lax.rem(f, N2)
        j = f // N2
        col = pl.ds(pl.multiple_of(j * FB, FB), FB)
        before = f + N2 - 1
        tb = lax.rem(before, N2)
        pp = lax.rem(before // N2 + 1, 2)
        w3j = w3[:, col]
        w4j = w4[col, :]
        for rc in range(T2 // RC):
            rows = pl.ds(pl.multiple_of(t * T2 + rc * RC, RC), RC)
            a = dot(hn[rows, :], w3j).astype(bf16).astype(f32)
            d = dot_nt(gn[rows, :], w4j)
            h, g = gelu_and_grad(a)
            uu[par][rc * RC:(rc + 1) * RC, :] = h.astype(bf16)
            uu[2 + par][rc * RC:(rc + 1) * RC, :] = (d * g).astype(bf16)
        b_part(gt, ht, tb, pp, 1 - par, None if par == 0 else tb == 0)

    def l2_pair(k, carry):
        for par in (0, 1):
            f = 2 * k + par
            comm(f)

            @pl.when(f >= 2)
            def _():
                da3_store(f - 2, par).wait()

            l2_trip(f, par)
            da3_store(f, par).start()
        return carry

    lax.fori_loop(0, NB * N2 // 2, l2_pair, 0)
    b_part(gt, ht, N2 - 1, (NB - 1) % 2, 1, None)
    for par in (0, 1):
        da3_store(NB * N2 - 2 + par, par).wait()

    def da3_load(i, par, cc):
        return pltpu.make_async_copy(
            da3_hbm.at[cc, pl.ds(i * T1, T1)],
            vv.at[2 * par + cc // 4, pl.ds((cc % 4) * T1, T1)],
            ld2_sem.at[par],
        )

    def da3_start(i, par):
        for cc in range(NB):
            da3_load(i, par, cc).start()
        x_copy(i).start()

    da3_start(0, 0)
    da3_start(1, 1)

    def dh2_pair(k, carry):
        comm(NB * N2 + k)
        for par in (0, 1):
            i = 2 * k + par
            for cc in range(NB):
                da3_load(i, par, cc).wait()
            x_copy(i).wait()
            rows = pl.ds(pl.multiple_of(i * T1, T1), T1)
            lanes = pl.ds(pl.multiple_of(lax.rem(i, 4) * T1, T1), T1)
            res = None
            for cc in range(NB):
                term = dot_nt(vv[2 * par + cc // 4, (cc % 4) * T1:(cc % 4 + 1) * T1, :], w3[:, cc * FB:(cc + 1) * FB])
                res = term if res is None else res + term
            dh2 = (res + gn[rows, :].astype(f32)).astype(bf16)
            hn[rows, :] = dh2
            ht[i // 4, :, lanes] = dh2.T
            gt[i // 4, :, lanes] = xs[lax.rem(i, 4)].T

            @pl.when(i + 2 < N1)
            def _():
                da3_start(i + 2, par)
        return carry

    lax.fori_loop(0, N1 // 2, dh2_pair, 0)

    base = NB * N2 + N1 // 2

    def a1_load(f):
        slot = lax.rem(f, 4)
        return pltpu.make_async_copy(
            a1_hbm.at[f // N2, pl.ds(lax.rem(f, N2) * T2, T2)], vv.at[slot], x_sem.at[slot])

    for f0 in range(3):
        a1_load(f0).start()

    def l1_trip(f, par):
        t = lax.rem(f, N2)
        j = f // N2
        col = pl.ds(pl.multiple_of(j * FB, FB), FB)
        before = f + N2 - 1
        tb = lax.rem(before, N2)
        pp = lax.rem(before // N2 + 1, 2)
        slot = lax.rem(f, 4)
        w2j = w2[col, :]
        for rc in range(T2 // RC):
            rows = pl.ds(pl.multiple_of(t * T2 + rc * RC, RC), RC)
            a = vv[slot, rc * RC:(rc + 1) * RC, :].astype(f32)
            d = dot_nt(hn[rows, :], w2j)
            h, g = gelu_and_grad(a)
            uu[par][rc * RC:(rc + 1) * RC, :] = h.astype(bf16)
            uu[2 + par][rc * RC:(rc + 1) * RC, :] = (d * g).astype(bf16)
        b_part(ht, gt, tb, pp, 1 - par, None if par == 0 else tb == 0)

    def l1_pair(k, carry):
        for par in (0, 1):
            f = 2 * k + par
            comm(base + f)

            @pl.when(f + 3 < NB * N2)
            def _():
                a1_load(f + 3).start()

            a1_load(f).wait()
            l1_trip(f, par)
        return carry

    lax.fori_loop(0, NB * N2 // 2, l1_pair, 0)
    comm(base + NB * N2)
    b_part(ht, gt, N2 - 1, (NB - 1) % 2, 1, None)

    def tail(k, carry):
        comm(base + NB * N2 + 1 + k)
        return carry

    lax.fori_loop(0, LAST_TRIP - base - NB * N2, tail, 0)


def finish_kernel(piece, o1, o2, o3, o4):
    p = pl.program_id(0)

    @pl.when(p < NB)
    def _():
        o3[...] = piece[0, 1]
        o4[...] = piece[0, 0].T

    @pl.when(p >= NB)
    def _():
        o1[...] = piece[0, 1]
        o2[...] = piece[0, 0].T


def device_step(x_loc, g_loc, w_one, w_two, w_three, w_four):
    any_spec = pl.BlockSpec(memory_space=pl.ANY)
    sums, _, _ = pl.pallas_call(
        kernel,
        name="grads",
        out_shape=(
            jax.ShapeDtypeStruct((2 * NB, 2, D, FB), f32),
            jax.ShapeDtypeStruct((NB, N, FB), bf16),
            jax.ShapeDtypeStruct((NB, N, FB), bf16),
        ),
        in_specs=[any_spec] * 6,
        out_specs=(any_spec,) * 3,
        scratch_shapes=[
            pltpu.VMEM((N, D), bf16),
            pltpu.VMEM((N2, D, T2), bf16),
            pltpu.VMEM((N, D), bf16),
            pltpu.VMEM((N2, D, T2), bf16),
            pltpu.VMEM((D, F), bf16),
            pltpu.VMEM((F, D), bf16),
            pltpu.VMEM((D, F), bf16),
            pltpu.VMEM((F, D), bf16),
            pltpu.VMEM((T2, FB), bf16),
            pltpu.VMEM((T2, FB), bf16),
            pltpu.VMEM((T2, FB), bf16),
            pltpu.VMEM((T2, FB), bf16),
            pltpu.VMEM((4, T2, FB), bf16),
            pltpu.VMEM((4, T1, D), bf16),
            pltpu.VMEM((2, 2, D, FB), f32),
            pltpu.VMEM((2, D, FB), f32),
            pltpu.VMEM((2, D, FB), f32),
            pltpu.VMEM((2, D // 2, FB), f32),
            pltpu.VMEM((2, D // 4, FB), f32),
            pltpu.VMEM((SLOTS, D, FB), f32),
            pltpu.SemaphoreType.DMA((5,)),
            pltpu.SemaphoreType.DMA((4,)),
            pltpu.SemaphoreType.DMA((2,)),
            pltpu.SemaphoreType.DMA((2,)),
            pltpu.SemaphoreType.DMA((SEMS, 6)),
            pltpu.SemaphoreType.DMA((SEMS, 6)),
            pltpu.SemaphoreType.DMA((SLOTS,)),
        ],
        compiler_params=pltpu.CompilerParams(
            collective_id=0, has_side_effects=True, vmem_limit_bytes=67000000),
        cost_estimate=pl.CostEstimate(flops=20 * N * D * F, bytes_accessed=200 << 20, transcendentals=3 * N * F),
    )(x_loc, g_loc, w_one, w_two, w_three, w_four)
    wide = jax.ShapeDtypeStruct((D, F), f32)
    tall = jax.ShapeDtypeStruct((F, D), f32)
    return pl.pallas_call(
        finish_kernel,
        name="finish",
        grid=(2 * NB,),
        out_shape=(wide, tall, wide, tall),
        in_specs=[pl.BlockSpec((1, 2, D, FB), lambda p: (p, 0, 0, 0))],
        out_specs=(
            pl.BlockSpec((D, FB), lambda p: (0, jnp.maximum(p - NB, 0))),
            pl.BlockSpec((FB, D), lambda p: (jnp.maximum(p - NB, 0), 0)),
            pl.BlockSpec((D, FB), lambda p: (0, jnp.minimum(p, NB - 1))),
            pl.BlockSpec((FB, D), lambda p: (jnp.minimum(p, NB - 1), 0)),
        ),
    )(sums)


def solution(mesh):
    batch_spec = P(("z", "y", "xc"), None)
    whole_spec = P(None, None)
    return jax.shard_map(
        device_step,
        mesh=mesh,
        in_specs=(batch_spec, batch_spec, whole_spec, whole_spec, whole_spec, whole_spec),
        out_specs=(whole_spec, whole_spec, whole_spec, whole_spec),
        check_vma=False,
    )
```

```python
import functools
import math

import jax
import jax.numpy as jnp
from jax import lax
from jax.experimental import pallas as pl
from jax.experimental.pallas import tpu as pltpu
from jax.sharding import PartitionSpec as P

MESH = pl.DeviceIdType.MESH
GELU_C = math.sqrt(2.0 / math.pi)
GELU_K = 0.044715

N = 8192
D = 512
F = 2048
FB = 256
NB = F // FB
T1 = 512
N1 = N // T1
RH = T1 // 2
T2 = 2048
N2 = N // T2
RC2 = 128
RC1 = 256
KU = 256
RA = 128
UNITS = 2 * (T2 // KU)
SLOTS = 4
SEMS = 8
OFFS = (0, 2, 6, 9, 12, 16, 18)
LAST_TRIP = 73 + OFFS[-1]

bf16 = jnp.bfloat16
f32 = jnp.float32


def dot(a, b):
    return jnp.dot(a, b, preferred_element_type=f32)


def gelu_half(a):
    sq = a * a
    t = jnp.tanh(a * (GELU_C + (GELU_C * GELU_K) * sq))
    s = 0.5 + 0.5 * t
    return sq, s, a * s


def gelu_and_grad(a):
    sq, s, h = gelu_half(a)
    g = s + (h * (1.0 - s)) * (2.0 * GELU_C + (6.0 * GELU_C * GELU_K) * sq)
    return h, g


def kernel(x_hbm, g_hbm, w1_hbm, w2_hbm, w3_hbm, w4_hbm, out, a1_hbm, da3_hbm,
           gn, gt, hn, ht, w1, w2, w3, w4, w4t, u0, u1, u2, u3, vv, xs,
           pacc, rx, sm, r1, r2, rs,
           ld_sem, x_sem, st_sem, ld2_sem, send_sem, recv_sem, loc_sem):
    z = lax.axis_index("z")
    y = lax.axis_index("y")
    c = lax.axis_index("xc")
    partner = (z, y, 1 - c)
    near_a = (lax.rem(z + c, 2), lax.rem(y + 1 - c, 2), c)
    near_b = (lax.rem(z + 1 - c, 2), lax.rem(y + c, 2), c)
    bit_a = y * (1 - c) + z * c
    bit_b = z * (1 - c) + y * c

    barrier = pltpu.get_barrier_semaphore()
    for dev in (partner, near_a, near_b):
        pl.semaphore_signal(barrier, inc=1, device_id=dev, device_id_type=MESH)

    def x_copy(i):
        slot = lax.rem(i, 4)
        return pltpu.make_async_copy(x_hbm.at[pl.ds(i * T1, T1)], xs.at[slot], x_sem.at[slot])

    loads = [
        pltpu.make_async_copy(w1_hbm, w1, ld_sem.at[0]),
        pltpu.make_async_copy(w2_hbm, w2, ld_sem.at[1]),
        pltpu.make_async_copy(g_hbm, gn, ld_sem.at[2]),
        pltpu.make_async_copy(w3_hbm, w3, ld_sem.at[3]),
        pltpu.make_async_copy(w4_hbm, w4, ld_sem.at[4]),
    ]
    loads[0].start()
    x_copy(0).start()
    x_copy(1).start()
    for ld in loads[1:]:
        ld.start()
    pl.semaphore_wait(barrier, 3)

    uu = (u0, u1, u2, u3)

    def a1_store(i, par, cc):
        return pltpu.make_async_copy(
            vv.at[2 * par + cc // 4, pl.ds((cc % 4) * T1, T1)],
            a1_hbm.at[cc, pl.ds(i * T1, T1)],
            st_sem.at[par],
        )

    def h1_part(par, m, cc):
        return uu[2 * par + cc // 4][(cc % 4) * T1 + m * RH:(cc % 4) * T1 + (m + 1) * RH, :]

    def h2_unit(par, m, cc, total):
        term = dot(h1_part(par, m, cc), w2[cc * FB:(cc + 1) * FB, :])
        return term if total is None else total + term

    def h2_store(i, m, total, x_rows):
        h2 = (total + x_rows.astype(f32)).astype(bf16)
        hn[pl.ds(pl.multiple_of(i * T1 + m * RH, RH), RH), :] = h2
        ht[i, :, m * RH:(m + 1) * RH] = h2.T

    def fwd_trip(i, par, with_a, with_b):
        xt = xs.at[lax.rem(i, 4)]
        xp = xs.at[lax.rem(i + 3, 4)]
        total = None
        chunks = NB * (T1 // RA)
        for n in range(chunks):
            if with_a:
                cc, r = n // (T1 // RA), n % (T1 // RA)
                a = dot(xt[r * RA:(r + 1) * RA, :], w1[:, cc * FB:(cc + 1) * FB]).astype(bf16)
                lo = (cc % 4) * T1 + r * RA
                vv[2 * par + cc // 4, lo:lo + RA, :] = a
                _, _, h = gelu_half(a.astype(f32))
                uu[2 * par + cc // 4][lo:lo + RA, :] = h.astype(bf16)
            if with_b:
                for n2 in range(n * 2 * NB // chunks, (n + 1) * 2 * NB // chunks):
                    m, cc = n2 // NB, n2 % NB
                    total = h2_unit(1 - par, m, cc, total if cc else None)
                    if cc == NB - 1:
                        h2_store(i - 1, m, total, xp[m * RH:(m + 1) * RH, :])
        if with_a:
            rows = pl.ds(pl.multiple_of(i * T1, T1), T1)
            gt[i] = gn[rows, :].T

    def fwd_tail_transposes(i):
        lanes = pl.ds(pl.multiple_of(i * (F // N1), F // N1), F // N1)
        w4t[:, lanes] = w4[lanes, :].T

    loads[0].wait()
    x_copy(0).wait()
    x_copy(2).start()
    loads[2].wait()
    fwd_trip(0, 0, True, False)
    for cc in range(NB):
        a1_store(0, 0, cc).start()
    for ld in (loads[1], loads[3], loads[4]):
        ld.wait()
    fwd_tail_transposes(0)

    def fwd_pair(k, carry):
        for par in (1, 0):
            i = 2 * k + 2 - par

            @pl.when(i >= 2)
            def _():
                for cc in range(NB):
                    a1_store(i - 2, par, cc).wait()

            @pl.when(i + 2 < N1)
            def _():
                x_copy(i + 2).start()

            x_copy(i).wait()
            fwd_trip(i, par, True, True)
            fwd_tail_transposes(i)
            for cc in range(NB):
                a1_store(i, par, cc).start()
        return carry

    lax.fori_loop(0, N1 // 2 - 1, fwd_pair, 0)
    for cc in range(NB):
        a1_store(N1 - 3, 1, cc).wait()
    x_copy(N1 - 1).wait()
    fwd_trip(N1 - 1, 1, True, True)
    fwd_tail_transposes(N1 - 1)
    for cc in range(NB):
        a1_store(N1 - 1, 1, cc).start()
    fwd_trip(N1, 0, False, True)
    for par in (0, 1):
        for cc in range(NB):
            a1_store(N1 - 2 + par, par, cc).wait()

    def half(b):
        return pl.ds(pl.multiple_of(b * (D // 2), D // 2), D // 2)

    def quarter(a, b):
        return pl.ds(pl.multiple_of(a * (D // 2) + b * (D // 4), D // 4), D // 4)

    def remote(src, dst, p, step, dev):
        e = lax.rem(p, SEMS)
        return pltpu.make_async_remote_copy(
            src_ref=src, dst_ref=dst, send_sem=send_sem.at[e, step], recv_sem=recv_sem.at[e, step],
            device_id=dev, device_id_type=MESH)

    def cp_pair(p):
        e = lax.rem(p, 2)
        return remote(pacc.at[e, 1 - c], rx.at[e], p, 0, partner)

    def cp_s1(p):
        e = lax.rem(p, 2)
        return remote(sm.at[e, half(1 - bit_a)], r1.at[e], p, 1, near_a)

    def cp_s2(p):
        e = lax.rem(p, 2)
        return remote(sm.at[e, quarter(bit_a, 1 - bit_b)], r2.at[e], p, 2, near_b)

    def cp_s3(p):
        part = rs.at[lax.rem(p, SLOTS), quarter(bit_a, bit_b)]
        return remote(part, part, p, 3, near_b)

    def cp_s4(p):
        part = rs.at[lax.rem(p, SLOTS), half(bit_a)]
        return remote(part, part, p, 4, near_a)

    def cp_s5(p):
        return remote(rs.at[lax.rem(p, SLOTS)], out.at[p, c], p, 5, partner)

    def cp_loc(p):
        e = lax.rem(p, SLOTS)
        return pltpu.make_async_copy(rs.at[e], out.at[p, c], loc_sem.at[e])

    def h_pair_send(p):
        cp_pair(p).start()

    def h_s1(p):
        cp_pair(p).wait()
        e = lax.rem(p, 2)
        sm[e] = pacc[e, c] + rx[e]
        cp_s1(p).start()

    def h_s2(p):
        cp_s1(p).wait()
        e = lax.rem(p, 2)
        rows = half(bit_a)
        sm[e, rows] = sm[e, rows] + r1[e]
        cp_s2(p).start()

    def h_s3(p):
        cp_s2(p).wait()
        e = lax.rem(p, 2)
        rows = quarter(bit_a, bit_b)
        rs[lax.rem(p, SLOTS), rows] = (sm[e, rows] + r2[e]) * 0.125
        cp_s3(p).start()

    def h_s4(p):
        cp_s3(p).wait()
        cp_s4(p).start()

    def h_s5(p):
        cp_s4(p).wait()
        cp_s5(p).start()
        cp_loc(p).start()

    def h_end(p):
        cp_s5(p).wait()
        cp_loc(p).wait()

    stages = (h_pair_send, h_s1, h_s2, h_s3, h_s4, h_s5, h_end)

    def comm(f):
        for order in (0, 6, 5, 4, 3, 2, 1):
            q = f + (40 - 5 - OFFS[order])
            k = q // 4 - 10
            ok = jnp.logical_and(
                lax.rem(q, 4) == 0,
                jnp.logical_or(jnp.logical_and(k >= 0, k < NB), jnp.logical_and(k >= NB + 2, k < 2 * NB + 2)))

            @pl.when(ok)
            def _():
                stages[order](k - 2 * (k // (NB + 2)))

    def b_unit(lhs0, lhs1, tb, par, pb, first, u, values):
        half_units = UNITS // 2
        m, kq = u // half_units, u % half_units
        rows = slice(m * (D // 2), (m + 1) * (D // 2))
        lo = kq * KU
        out_values = []
        for idx, lhs in ((0, lhs0), (1, lhs1)):
            value = values[idx] if kq else None
            term = dot(lhs[tb * (T2 // T1) + lo // T1, rows, lo % T1:lo % T1 + KU], uu[2 * idx + pb][lo:lo + KU, :])
            value = term if value is None else value + term
            if kq == half_units - 1:
                old = pacc[par, idx, rows, :]
                if first is not None:
                    old = jnp.where(first, 0.0, old)
                pacc[par, idx, rows, :] = old + value
            out_values.append(value)
        return out_values

    def b_some(lhs0, lhs1, tb, par, pb, first, rc, chunks, values):
        for u in range(rc * UNITS // chunks, (rc + 1) * UNITS // chunks):
            values = b_unit(lhs0, lhs1, tb, par, pb, first, u, values)
        return values

    def b_part(lhs0, lhs1, tb, par, pb, first):
        values = None
        for u in range(UNITS):
            values = b_unit(lhs0, lhs1, tb, par, pb, first, u, values)

    def da3_store(f, par):
        return pltpu.make_async_copy(
            uu[2 + par], da3_hbm.at[f // N2, pl.ds(lax.rem(f, N2) * T2, T2)], st_sem.at[par])

    def l2_trip(f, par):
        t = lax.rem(f, N2)
        j = f // N2
        col = pl.ds(pl.multiple_of(j * FB, FB), FB)
        before = f + N2 - 1
        tb = lax.rem(before, N2)
        pp = lax.rem(before // N2 + 1, 2)
        w3j = w3[:, col]
        w4j = w4t[:, col]
        values = None
        for rc in range(T2 // RC2):
            rows = pl.ds(pl.multiple_of(t * T2 + rc * RC2, RC2), RC2)
            a = dot(hn[rows, :], w3j).astype(bf16).astype(f32)
            d = dot(gn[rows, :], w4j)
            h, g = gelu_and_grad(a)
            uu[par][rc * RC2:(rc + 1) * RC2, :] = h.astype(bf16)
            uu[2 + par][rc * RC2:(rc + 1) * RC2, :] = (d * g).astype(bf16)
            values = b_some(gt, ht, tb, pp, 1 - par, None if par == 0 else tb == 0, rc, T2 // RC2, values)

    def l2_pair(k, carry):
        for par in (0, 1):
            f = 2 * k + par
            comm(f)

            @pl.when(f >= 2)
            def _():
                da3_store(f - 2, par).wait()

            l2_trip(f, par)
            da3_store(f, par).start()
        return carry

    lax.fori_loop(0, NB * N2 // 2, l2_pair, 0)
    b_part(gt, ht, N2 - 1, (NB - 1) % 2, 1, None)
    for par in (0, 1):
        da3_store(NB * N2 - 2 + par, par).wait()

    def da3_load(i, par, cc):
        return pltpu.make_async_copy(
            da3_hbm.at[cc, pl.ds(i * T1, T1)],
            vv.at[2 * par + cc // 4, pl.ds((cc % 4) * T1, T1)],
            ld2_sem.at[par],
        )

    def da3_start(i, par):
        for cc in range(NB):
            da3_load(i, par, cc).start()
        x_copy(i).start()

    da3_start(0, 0)
    da3_start(1, 1)
    for cc in range(NB):
        cols = slice(cc * FB, (cc + 1) * FB)
        w4[cols, :] = w3[:, cols].T
        w4t[:, cols] = w2[cols, :].T

    def dh2_pair(k, carry):
        comm(NB * N2 + k)
        for par in (0, 1):
            i = 2 * k + par
            for cc in range(NB):
                da3_load(i, par, cc).wait()
            x_copy(i).wait()
            for m in (0, 1):
                rows = pl.ds(pl.multiple_of(i * T1 + m * RH, RH), RH)
                total = None
                for cc in range(NB):
                    lo = (cc % 4) * T1 + m * RH
                    term = dot(vv[2 * par + cc // 4, lo:lo + RH, :], w4[cc * FB:(cc + 1) * FB, :])
                    total = term if total is None else total + term
                dh2 = (total + gn[rows, :].astype(f32)).astype(bf16)
                hn[rows, :] = dh2
                ht[i, :, m * RH:(m + 1) * RH] = dh2.T
            gt[i] = xs[lax.rem(i, 4)].T

            @pl.when(i + 2 < N1)
            def _():
                da3_start(i + 2, par)
        return carry

    lax.fori_loop(0, N1 // 2, dh2_pair, 0)

    base = NB * N2 + N1 // 2

    def a1_load(f):
        slot = lax.rem(f, 4)
        return pltpu.make_async_copy(
            a1_hbm.at[f // N2, pl.ds(lax.rem(f, N2) * T2, T2)], vv.at[slot], x_sem.at[slot])

    for f0 in range(3):
        a1_load(f0).start()

    def l1_trip(f, par):
        t = lax.rem(f, N2)
        j = f // N2
        col = pl.ds(pl.multiple_of(j * FB, FB), FB)
        before = f + N2 - 1
        tb = lax.rem(before, N2)
        pp = lax.rem(before // N2 + 1, 2)
        slot = lax.rem(f, 4)
        w2j = w4t[:, col]
        values = None
        for rc in range(T2 // RC1):
            rows = pl.ds(pl.multiple_of(t * T2 + rc * RC1, RC1), RC1)
            a = vv[slot, rc * RC1:(rc + 1) * RC1, :].astype(f32)
            d = dot(hn[rows, :], w2j)
            h, g = gelu_and_grad(a)
            uu[par][rc * RC1:(rc + 1) * RC1, :] = h.astype(bf16)
            uu[2 + par][rc * RC1:(rc + 1) * RC1, :] = (d * g).astype(bf16)
            values = b_some(ht, gt, tb, pp, 1 - par, None if par == 0 else tb == 0, rc, T2 // RC1, values)

    def l1_pair(k, carry):
        for par in (0, 1):
            f = 2 * k + par
            comm(base + f)

            @pl.when(f + 3 < NB * N2)
            def _():
                a1_load(f + 3).start()

            a1_load(f).wait()
            l1_trip(f, par)
        return carry

    lax.fori_loop(0, NB * N2 // 2, l1_pair, 0)
    comm(base + NB * N2)
    b_part(ht, gt, N2 - 1, (NB - 1) % 2, 1, None)

    def tail(k, carry):
        comm(base + NB * N2 + 1 + k)
        return carry

    lax.fori_loop(0, LAST_TRIP - base - NB * N2, tail, 0)


def finish_kernel(sums, o1, o2, o3, o4, buf, flip, in_sem, wide_sem, tall_sem):
    def load(p):
        return pltpu.make_async_copy(sums.at[p], buf.at[p], in_sem.at[p])

    def store_wide(o, j, p):
        return pltpu.make_async_copy(
            buf.at[p, 1], o.at[:, pl.ds(pl.multiple_of(j * FB, FB), FB)], wide_sem.at[p])

    def store_tall(o, j, p):
        return pltpu.make_async_copy(
            flip.at[p], o.at[pl.ds(pl.multiple_of(j * FB, FB), FB), :], tall_sem.at[p])

    for p in range(2 * NB):
        load(p).start()
    for base, wide, tall in ((0, o3, o4), (NB, o1, o2)):
        def step(j, carry):
            p = base + j
            load(p).wait()
            store_wide(wide, j, p).start()
            flip[p] = buf[p, 0].T
            store_tall(tall, j, p).start()
            return carry
        lax.fori_loop(0, NB, step, 0)
    for base, wide, tall in ((0, o3, o4), (NB, o1, o2)):
        def drain(j, carry):
            store_wide(wide, j, base + j).wait()
            store_tall(tall, j, base + j).wait()
            return carry
        lax.fori_loop(0, NB, drain, 0)


def device_step(x_loc, g_loc, w_one, w_two, w_three, w_four):
    any_spec = pl.BlockSpec(memory_space=pl.ANY)
    sums, _, _ = pl.pallas_call(
        kernel,
        name="grads",
        out_shape=(
            jax.ShapeDtypeStruct((2 * NB, 2, D, FB), f32),
            jax.ShapeDtypeStruct((NB, N, FB), bf16),
            jax.ShapeDtypeStruct((NB, N, FB), bf16),
        ),
        in_specs=[any_spec] * 6,
        out_specs=(any_spec,) * 3,
        scratch_shapes=[
            pltpu.VMEM((N, D), bf16),
            pltpu.VMEM((N1, D, T1), bf16),
            pltpu.VMEM((N, D), bf16),
            pltpu.VMEM((N1, D, T1), bf16),
            pltpu.VMEM((D, F), bf16),
            pltpu.VMEM((F, D), bf16),
            pltpu.VMEM((D, F), bf16),
            pltpu.VMEM((F, D), bf16),
            pltpu.VMEM((D, F), bf16),
            pltpu.VMEM((T2, FB), bf16),
            pltpu.VMEM((T2, FB), bf16),
            pltpu.VMEM((T2, FB), bf16),
            pltpu.VMEM((T2, FB), bf16),
            pltpu.VMEM((4, T2, FB), bf16),
            pltpu.VMEM((4, T1, D), bf16),
            pltpu.VMEM((2, 2, D, FB), f32),
            pltpu.VMEM((2, D, FB), f32),
            pltpu.VMEM((2, D, FB), f32),
            pltpu.VMEM((2, D // 2, FB), f32),
            pltpu.VMEM((2, D // 4, FB), f32),
            pltpu.VMEM((SLOTS, D, FB), f32),
            pltpu.SemaphoreType.DMA((5,)),
            pltpu.SemaphoreType.DMA((4,)),
            pltpu.SemaphoreType.DMA((2,)),
            pltpu.SemaphoreType.DMA((2,)),
            pltpu.SemaphoreType.DMA((SEMS, 6)),
            pltpu.SemaphoreType.DMA((SEMS, 6)),
            pltpu.SemaphoreType.DMA((SLOTS,)),
        ],
        compiler_params=pltpu.CompilerParams(
            collective_id=0, has_side_effects=True, vmem_limit_bytes=67000000),
        cost_estimate=pl.CostEstimate(flops=20 * N * D * F, bytes_accessed=200 << 20, transcendentals=3 * N * F),
    )(x_loc, g_loc, w_one, w_two, w_three, w_four)
    wide = jax.ShapeDtypeStruct((D, F), f32)
    tall = jax.ShapeDtypeStruct((F, D), f32)
    return pl.pallas_call(
        finish_kernel,
        name="finish",
        out_shape=(wide, tall, wide, tall),
        in_specs=[any_spec],
        out_specs=(any_spec,) * 4,
        scratch_shapes=[
            pltpu.VMEM((2 * NB, 2, D, FB), f32),
            pltpu.VMEM((2 * NB, FB, D), f32),
            pltpu.SemaphoreType.DMA((2 * NB,)),
            pltpu.SemaphoreType.DMA((2 * NB,)),
            pltpu.SemaphoreType.DMA((2 * NB,)),
        ],
        compiler_params=pltpu.CompilerParams(vmem_limit_bytes=40 << 20),
    )(sums)


def solution(mesh):
    batch_spec = P(("z", "y", "xc"), None)
    whole_spec = P(None, None)
    return jax.shard_map(
        device_step,
        mesh=mesh,
        in_specs=(batch_spec, batch_spec, whole_spec, whole_spec, whole_spec, whole_spec),
        out_specs=(whole_spec, whole_spec, whole_spec, whole_spec),
        check_vma=False,
    )
```

```python
import functools
import math

import jax
import jax.numpy as jnp
from jax import lax
from jax.experimental import pallas as pl
from jax.experimental.pallas import tpu as pltpu
from jax.sharding import PartitionSpec as P

MESH = pl.DeviceIdType.MESH
GELU_C = math.sqrt(2.0 / math.pi)
GELU_K = 0.044715

N = 8192
D = 512
F = 2048
FB = 256
NB = F // FB
T1 = 512
N1 = N // T1
RH = T1 // 2
T2 = 2048
N2 = N // T2
RC2 = 128
RC1 = 256
KU = 256
RA = 128
UNITS = 2 * (T2 // KU)
TQ = T2 // T1
SLOTS = 4
SEMS = 8
OFFS = {2: (0, 2, 6, 10, 12, 16, 18), 1: (0, 1, 5, 8, 11, 15, 16)}
BASE = {2: 6, 1: 4 * (NB + 2) + 5}
LAST_TRIP = BASE[1] + 4 * (NB - 1) + OFFS[1][-1]

bf16 = jnp.bfloat16
f32 = jnp.float32


def dot(a, b):
    return jnp.dot(a, b, preferred_element_type=f32)


def gelu_half(a):
    sq = a * a
    t = jnp.tanh(a * (GELU_C + (GELU_C * GELU_K) * sq))
    s = 0.5 + 0.5 * t
    return sq, s, a * s


def gelu_and_grad(a):
    sq, s, h = gelu_half(a)
    g = s + (h * (1.0 - s)) * (2.0 * GELU_C + (6.0 * GELU_C * GELU_K) * sq)
    return h, g


def kernel(x_hbm, g_hbm, w1_hbm, w2_hbm, w3_hbm, w4_hbm, out, a1_hbm, da3_hbm,
           gn, gt, hn, ht, w1, w2, w3, w4, w4t, u0, u1, d0, d1, va, vb, xs,
           pacc, rx, sm, r1, r2, rs,
           ld_sem, x_sem, st_sem, ld2_sem, send_sem, recv_sem, loc_sem):
    z = lax.axis_index("z")
    y = lax.axis_index("y")
    c = lax.axis_index("xc")
    partner = (z, y, 1 - c)
    near_a = (lax.rem(z + c, 2), lax.rem(y + 1 - c, 2), c)
    near_b = (lax.rem(z + 1 - c, 2), lax.rem(y + c, 2), c)
    bit_a = y * (1 - c) + z * c
    bit_b = z * (1 - c) + y * c

    barrier = pltpu.get_barrier_semaphore()
    for dev in (partner, near_a, near_b):
        pl.semaphore_signal(barrier, inc=1, device_id=dev, device_id_type=MESH)

    def x_copy(i):
        slot = lax.rem(i, 4)
        return pltpu.make_async_copy(x_hbm.at[pl.ds(i * T1, T1)], xs.at[slot], x_sem.at[slot])

    loads = [
        pltpu.make_async_copy(w1_hbm, w1, ld_sem.at[0]),
        pltpu.make_async_copy(w2_hbm, w2, ld_sem.at[1]),
        pltpu.make_async_copy(g_hbm, gn, ld_sem.at[2]),
        pltpu.make_async_copy(w3_hbm, w3, ld_sem.at[3]),
        pltpu.make_async_copy(w4_hbm, w4, ld_sem.at[4]),
    ]
    loads[0].start()
    x_copy(0).start()
    x_copy(1).start()
    for ld in loads[1:]:
        ld.start()

    hs = (u0, u1)
    ds = (d0, d1)
    vs = (va, vb)

    def a1_store(i, par):
        return pltpu.make_async_copy(vs[par], a1_hbm.at[:, i], st_sem.at[par])

    def h1_tile(par, cc):
        return hs[cc // 4].at[cc % 4] if par == 0 else ds[cc // 4].at[cc % 4]

    def h2_unit(par, m, cc, total):
        term = dot(h1_tile(par, cc)[m * RH:(m + 1) * RH, :], w2[cc * FB:(cc + 1) * FB, :])
        return term if total is None else total + term

    def h2_store(i, m, total, x_rows):
        h2 = (total + x_rows.astype(f32)).astype(bf16)
        hn[pl.ds(pl.multiple_of(i * T1 + m * RH, RH), RH), :] = h2
        ht[i, :, m * RH:(m + 1) * RH] = h2.T

    def fwd_trip(i, par, with_a, with_b, with_gt=True):
        xt = xs.at[lax.rem(i, 4)]
        xp = xs.at[lax.rem(i + 3, 4)]
        total = None
        chunks = NB * (T1 // RA)
        for n in range(chunks):
            if with_a:
                cc, r = n // (T1 // RA), n % (T1 // RA)
                a = dot(xt[r * RA:(r + 1) * RA, :], w1[:, cc * FB:(cc + 1) * FB]).astype(bf16)
                vs[par][cc, r * RA:(r + 1) * RA, :] = a
                _, _, h = gelu_half(a.astype(f32))
                h1_tile(par, cc)[r * RA:(r + 1) * RA, :] = h.astype(bf16)
            if with_b:
                for n2 in range(n * 2 * NB // chunks, (n + 1) * 2 * NB // chunks):
                    m, cc = n2 // NB, n2 % NB
                    total = h2_unit(1 - par, m, cc, total if cc else None)
                    if cc == NB - 1:
                        h2_store(i - 1, m, total, xp[m * RH:(m + 1) * RH, :])
        if with_a and with_gt:
            rows = pl.ds(pl.multiple_of(i * T1, T1), T1)
            gt[i] = gn[rows, :].T

    def fwd_tail_transposes(i):
        lanes = pl.ds(pl.multiple_of(i * (F // N1), F // N1), F // N1)
        w4t[:, lanes] = w4[lanes, :].T

    loads[0].wait()
    x_copy(0).wait()
    x_copy(2).start()
    fwd_trip(0, 0, True, False, False)
    a1_store(0, 0).start()
    for ld in loads[1:]:
        ld.wait()
    gt[0] = gn[:T1, :].T
    fwd_tail_transposes(0)

    def fwd_pair(k, carry):
        for par in (1, 0):
            i = 2 * k + 2 - par

            @pl.when(i >= 2)
            def _():
                a1_store(i - 2, par).wait()

            @pl.when(i + 2 < N1)
            def _():
                x_copy(i + 2).start()

            x_copy(i).wait()
            fwd_trip(i, par, True, True)
            fwd_tail_transposes(i)
            a1_store(i, par).start()
        return carry

    lax.fori_loop(0, N1 // 2 - 1, fwd_pair, 0)
    a1_store(N1 - 3, 1).wait()
    x_copy(N1 - 1).wait()
    fwd_trip(N1 - 1, 1, True, True)
    fwd_tail_transposes(N1 - 1)
    a1_store(N1 - 1, 1).start()
    fwd_trip(N1, 0, False, True)
    for par in (0, 1):
        a1_store(N1 - 2 + par, par).wait()

    pl.semaphore_wait(barrier, 3)

    def half(b):
        return pl.ds(pl.multiple_of(b * (D // 2), D // 2), D // 2)

    def quarter(a, b):
        return pl.ds(pl.multiple_of(a * (D // 2) + b * (D // 4), D // 4), D // 4)

    def remote(src, dst, p, step, dev):
        e = lax.rem(p, SEMS)
        return pltpu.make_async_remote_copy(
            src_ref=src, dst_ref=dst, send_sem=send_sem.at[e, step], recv_sem=recv_sem.at[e, step],
            device_id=dev, device_id_type=MESH)

    def cp_pair(p):
        e = lax.rem(p, 2)
        return remote(pacc.at[e, 1 - c], rx.at[e], p, 0, partner)

    def cp_s1(p):
        e = lax.rem(p, 2)
        return remote(sm.at[e, half(1 - bit_a)], r1.at[e], p, 1, near_a)

    def cp_s2(p):
        e = lax.rem(p, 2)
        return remote(sm.at[e, quarter(bit_a, 1 - bit_b)], r2.at[e], p, 2, near_b)

    def cp_s3(p):
        part = rs.at[lax.rem(p, SLOTS), quarter(bit_a, bit_b)]
        return remote(part, part, p, 3, near_b)

    def cp_s4(p):
        part = rs.at[lax.rem(p, SLOTS), half(bit_a)]
        return remote(part, part, p, 4, near_a)

    def cp_s5(p):
        return remote(rs.at[lax.rem(p, SLOTS)], out.at[p, c], p, 5, partner)

    def cp_loc(p):
        e = lax.rem(p, SLOTS)
        return pltpu.make_async_copy(rs.at[e], out.at[p, c], loc_sem.at[e])

    def h_pair_send(p):
        cp_pair(p).start()

    def h_s1(p):
        cp_pair(p).wait()
        e = lax.rem(p, 2)
        sm[e] = pacc[e, c] + rx[e]
        cp_s1(p).start()

    def h_s2(p):
        cp_s1(p).wait()
        e = lax.rem(p, 2)
        rows = half(bit_a)
        sm[e, rows] = sm[e, rows] + r1[e]
        cp_s2(p).start()

    def h_s3(p):
        cp_s2(p).wait()
        e = lax.rem(p, 2)
        rows = quarter(bit_a, bit_b)
        rs[lax.rem(p, SLOTS), rows] = (sm[e, rows] + r2[e]) * 0.125
        cp_s3(p).start()

    def h_s4(p):
        cp_s3(p).wait()
        cp_s4(p).start()

    def h_s5(p):
        cp_s4(p).wait()
        cp_s5(p).start()
        cp_loc(p).start()

    def h_end(p):
        cp_s5(p).wait()
        cp_loc(p).wait()

    stages = (h_pair_send, h_s1, h_s2, h_s3, h_s4, h_s5, h_end)

    def comm(layer, f, parity):
        for order in (0, 6, 5, 4, 3, 2, 1):
            due = BASE[layer] + OFFS[layer][order]
            if (due - parity) % 2:
                continue
            q = f + (64 - due)
            k = q // 4 - 16

            @pl.when(jnp.logical_and(lax.rem(q, 4) == 0, jnp.logical_and(k >= 0, k < NB)))
            def _():
                stages[order](k if layer == 2 else k + NB)

    def b_unit(lhs0, lhs1, tb, par, rhs, first, u, values):
        half_units = UNITS // 2
        m, kq = u // half_units, u % half_units
        rows = slice(m * (D // 2), (m + 1) * (D // 2))
        lo = kq * KU
        out_values = []
        for idx, lhs in ((0, lhs0), (1, lhs1)):
            value = values[idx] if kq else None
            term = dot(lhs[tb * (T2 // T1) + lo // T1, rows, lo % T1:lo % T1 + KU], rhs[idx][lo // T1, lo % T1:lo % T1 + KU, :])
            value = term if value is None else value + term
            if kq == half_units - 1:
                old = pacc[par, idx, rows, :]
                if first is not None:
                    old = jnp.where(first, 0.0, old)
                pacc[par, idx, rows, :] = old + value
            out_values.append(value)
        return out_values

    def b_some(lhs0, lhs1, tb, par, rhs, first, rc, chunks, values):
        for u in range(rc * UNITS // chunks, (rc + 1) * UNITS // chunks):
            values = b_unit(lhs0, lhs1, tb, par, rhs, first, u, values)
        return values

    def b_part(lhs0, lhs1, tb, par, rhs, between=None):
        values = None
        for u in range(UNITS):
            values = b_unit(lhs0, lhs1, tb, par, rhs, None, u, values)
            if between is not None and u % 2 == 1:
                between(u // 2)

    def da3_store(f, par, e):
        return pltpu.make_async_copy(
            vs[par].at[pl.ds(e * TQ, TQ)], da3_hbm.at[f // N2, pl.ds(lax.rem(f, N2) * TQ, TQ)], st_sem.at[2 * e + par])

    def l2_trip(f, par, e):
        t = lax.rem(f, N2)
        j = f // N2
        col = pl.ds(pl.multiple_of(j * FB, FB), FB)
        before = f + N2 - 1
        tb = lax.rem(before, N2)
        pp = lax.rem(before // N2 + 1, 2)
        w3j = w3[:, col]
        w4j = w4t[:, col]
        rhs = (hs[1 - par], vb.at[pl.ds((1 - e) * TQ, TQ)] if par == 0 else va.at[pl.ds(e * TQ, TQ)])
        values = None
        for rc in range(T2 // RC2):
            rows = pl.ds(pl.multiple_of(t * T2 + rc * RC2, RC2), RC2)
            tile, lo = rc * RC2 // T1, rc * RC2 % T1
            a = dot(hn[rows, :], w3j).astype(bf16).astype(f32)
            d = dot(gn[rows, :], w4j)
            h, g = gelu_and_grad(a)
            hs[par][tile, lo:lo + RC2, :] = h.astype(bf16)
            vs[par][e * TQ + tile, lo:lo + RC2, :] = (d * g).astype(bf16)
            values = b_some(gt, ht, tb, pp, rhs, None if par == 0 else tb == 0, rc, T2 // RC2, values)

    def l2_pair(k, carry):
        e = lax.rem(k, 2)
        comm(2, 2 * k, 0)

        @pl.when(k >= 2)
        def _():
            for par in (0, 1):
                da3_store(2 * k - 4 + par, par, e).wait()

        for par in (0, 1):
            l2_trip(2 * k + par, par, e)
        for par in (0, 1):
            da3_store(2 * k + par, par, e).start()
        return carry

    lax.fori_loop(0, NB * N2 // 2, l2_pair, 0)

    tiles = ((va, vb), ((u0, u1), (d0, d1)))

    def da3_loads(i, e, par):
        tile = tiles[e][par]
        if e == 0:
            return [pltpu.make_async_copy(da3_hbm.at[:, i], tile, ld2_sem.at[par])]
        return [
            pltpu.make_async_copy(da3_hbm.at[pl.ds(h * TQ, TQ), i], tile[h], ld2_sem.at[2 + 2 * par + h])
            for h in (0, 1)]

    def da3_tile(e, par, cc):
        return tiles[0][par].at[cc] if e == 0 else tiles[1][par][cc // 4].at[cc % 4]

    def da3_start(i, e, par):
        for ld in da3_loads(i, e, par):
            ld.start()
        x_copy(i).start()

    def turn_weights(cc):
        cols = slice(cc * FB, (cc + 1) * FB)
        w4[cols, :] = w3[:, cols].T
        w4t[:, cols] = w2[cols, :].T

    for f0 in range(NB * N2 - 4, NB * N2):
        da3_store(f0, f0 % 2, f0 // 2 % 2).wait()
    da3_start(0, 0, 0)
    b_part(gt, ht, N2 - 1, (NB - 1) % 2, (hs[1], vb.at[pl.ds(TQ, TQ)]), turn_weights)
    da3_start(1, 0, 1)
    da3_start(2, 1, 0)
    da3_start(3, 1, 1)

    def dh2_tile(i, e, par):
        for m in (0, 1):
            rows = pl.ds(pl.multiple_of(i * T1 + m * RH, RH), RH)
            total = None
            for cc in range(NB):
                term = dot(da3_tile(e, par, cc)[m * RH:(m + 1) * RH, :], w4[cc * FB:(cc + 1) * FB, :])
                total = term if total is None else total + term
            dh2 = (total + gn[rows, :].astype(f32)).astype(bf16)
            hn[rows, :] = dh2
            ht[i, :, m * RH:(m + 1) * RH] = dh2.T
        gt[i] = xs[lax.rem(i, 4)].T

    def dh2_four(q, carry):
        comm(2, NB * N2 + 2 * q, 0)
        for e in (0, 1):
            for par in (0, 1):
                i = 4 * q + 2 * e + par
                for ld in da3_loads(i, e, par):
                    ld.wait()
                x_copy(i).wait()
            for par in (0, 1):
                dh2_tile(4 * q + 2 * e + par, e, par)

            @pl.when(q < N1 // 4 - 1)
            def _():
                for par in (0, 1):
                    da3_start(4 * q + 4 + 2 * e + par, e, par)
        return carry

    lax.fori_loop(0, N1 // 4, dh2_four, 0)

    base = NB * N2 + N1 // 2

    def a1_load(k, par):
        f = 2 * k + par
        e = lax.rem(k, 2)
        return pltpu.make_async_copy(
            a1_hbm.at[f // N2, pl.ds(lax.rem(f, N2) * TQ, TQ)], vs[par].at[pl.ds(e * TQ, TQ)], x_sem.at[2 * e + par])

    for par in (0, 1):
        a1_load(0, par).start()

    def l1_trip(f, par):
        t = lax.rem(f, N2)
        j = f // N2
        col = pl.ds(pl.multiple_of(j * FB, FB), FB)
        before = f + N2 - 1
        tb = lax.rem(before, N2)
        pp = lax.rem(before // N2 + 1, 2)
        e = lax.rem(f // 2, 2)
        w2j = w4t[:, col]
        rhs = (hs[1 - par], ds[1 - par])
        values = None
        for rc in range(T2 // RC1):
            rows = pl.ds(pl.multiple_of(t * T2 + rc * RC1, RC1), RC1)
            tile, lo = rc * RC1 // T1, rc * RC1 % T1
            a = vs[par][e * TQ + tile, lo:lo + RC1, :].astype(f32)
            d = dot(hn[rows, :], w2j)
            h, g = gelu_and_grad(a)
            hs[par][tile, lo:lo + RC1, :] = h.astype(bf16)
            ds[par][tile, lo:lo + RC1, :] = (d * g).astype(bf16)
            values = b_some(ht, gt, tb, pp, rhs, None if par == 0 else tb == 0, rc, T2 // RC1, values)

    def l1_pair(k, carry):
        for par in (0, 1):
            f = base + 2 * k + par
            comm(2, f, par)
            comm(1, f, par)
            a1_load(k, par).wait()

            @pl.when(2 * k + 2 < NB * N2)
            def _():
                a1_load(k + 1, par).start()

            l1_trip(2 * k + par, par)
        return carry

    lax.fori_loop(0, NB * N2 // 2, l1_pair, 0)
    comm(1, base + NB * N2, 0)
    b_part(ht, gt, N2 - 1, (NB - 1) % 2, (hs[1], ds[1]))

    def tail(k, carry):
        for par in (1, 0):
            comm(1, base + NB * N2 + 2 + 2 * k - par, par)
        return carry

    lax.fori_loop(0, (LAST_TRIP - base - NB * N2 + 1) // 2, tail, 0)


def finish_kernel(sums, o1, o2, o3, o4, buf, flip, in_sem, wide_sem, tall_sem):
    def load(p):
        return pltpu.make_async_copy(sums.at[p], buf.at[p], in_sem.at[p])

    def store_wide(o, j, p):
        return pltpu.make_async_copy(
            buf.at[p, 1], o.at[:, pl.ds(pl.multiple_of(j * FB, FB), FB)], wide_sem.at[p])

    def store_tall(o, j, p):
        return pltpu.make_async_copy(
            flip.at[p], o.at[pl.ds(pl.multiple_of(j * FB, FB), FB), :], tall_sem.at[p])

    for p in range(2 * NB):
        load(p).start()
    for base, wide, tall in ((0, o3, o4), (NB, o1, o2)):
        def step(j, carry):
            p = base + j
            load(p).wait()
            store_wide(wide, j, p).start()
            flip[p] = buf[p, 0].T
            store_tall(tall, j, p).start()
            return carry
        lax.fori_loop(0, NB, step, 0)
    for base, wide, tall in ((0, o3, o4), (NB, o1, o2)):
        def drain(j, carry):
            store_wide(wide, j, base + j).wait()
            store_tall(tall, j, base + j).wait()
            return carry
        lax.fori_loop(0, NB, drain, 0)


def device_step(x_loc, g_loc, w_one, w_two, w_three, w_four):
    any_spec = pl.BlockSpec(memory_space=pl.ANY)
    sums, _, _ = pl.pallas_call(
        kernel,
        name="grads",
        out_shape=(
            jax.ShapeDtypeStruct((2 * NB, 2, D, FB), f32),
            jax.ShapeDtypeStruct((NB, N1, T1, FB), bf16),
            jax.ShapeDtypeStruct((NB, N1, T1, FB), bf16),
        ),
        in_specs=[any_spec] * 6,
        out_specs=(any_spec,) * 3,
        scratch_shapes=[
            pltpu.VMEM((N, D), bf16),
            pltpu.VMEM((N1, D, T1), bf16),
            pltpu.VMEM((N, D), bf16),
            pltpu.VMEM((N1, D, T1), bf16),
            pltpu.VMEM((D, F), bf16),
            pltpu.VMEM((F, D), bf16),
            pltpu.VMEM((D, F), bf16),
            pltpu.VMEM((F, D), bf16),
            pltpu.VMEM((D, F), bf16),
            pltpu.VMEM((TQ, T1, FB), bf16),
            pltpu.VMEM((TQ, T1, FB), bf16),
            pltpu.VMEM((TQ, T1, FB), bf16),
            pltpu.VMEM((TQ, T1, FB), bf16),
            pltpu.VMEM((NB, T1, FB), bf16),
            pltpu.VMEM((NB, T1, FB), bf16),
            pltpu.VMEM((4, T1, D), bf16),
            pltpu.VMEM((2, 2, D, FB), f32),
            pltpu.VMEM((2, D, FB), f32),
            pltpu.VMEM((2, D, FB), f32),
            pltpu.VMEM((2, D // 2, FB), f32),
            pltpu.VMEM((2, D // 4, FB), f32),
            pltpu.VMEM((SLOTS, D, FB), f32),
            pltpu.SemaphoreType.DMA((5,)),
            pltpu.SemaphoreType.DMA((4,)),
            pltpu.SemaphoreType.DMA((4,)),
            pltpu.SemaphoreType.DMA((6,)),
            pltpu.SemaphoreType.DMA((SEMS, 6)),
            pltpu.SemaphoreType.DMA((SEMS, 6)),
            pltpu.SemaphoreType.DMA((SLOTS,)),
        ],
        compiler_params=pltpu.CompilerParams(
            collective_id=0, has_side_effects=True, vmem_limit_bytes=67000000),
        cost_estimate=pl.CostEstimate(flops=20 * N * D * F, bytes_accessed=200 << 20, transcendentals=3 * N * F),
    )(x_loc, g_loc, w_one, w_two, w_three, w_four)
    wide = jax.ShapeDtypeStruct((D, F), f32)
    tall = jax.ShapeDtypeStruct((F, D), f32)
    return pl.pallas_call(
        finish_kernel,
        name="finish",
        out_shape=(wide, tall, wide, tall),
        in_specs=[any_spec],
        out_specs=(any_spec,) * 4,
        scratch_shapes=[
            pltpu.VMEM((2 * NB, 2, D, FB), f32),
            pltpu.VMEM((2 * NB, FB, D), f32),
            pltpu.SemaphoreType.DMA((2 * NB,)),
            pltpu.SemaphoreType.DMA((2 * NB,)),
            pltpu.SemaphoreType.DMA((2 * NB,)),
        ],
        compiler_params=pltpu.CompilerParams(vmem_limit_bytes=40 << 20),
    )(sums)


def solution(mesh):
    batch_spec = P(("z", "y", "xc"), None)
    whole_spec = P(None, None)
    return jax.shard_map(
        device_step,
        mesh=mesh,
        in_specs=(batch_spec, batch_spec, whole_spec, whole_spec, whole_spec, whole_spec),
        out_specs=(whole_spec, whole_spec, whole_spec, whole_spec),
        check_vma=False,
    )
```

```python
import functools
import math

import jax
import jax.numpy as jnp
from jax import lax
from jax.experimental import pallas as pl
from jax.experimental.pallas import tpu as pltpu
from jax.sharding import PartitionSpec as P

MESH = pl.DeviceIdType.MESH
GELU_C = math.sqrt(2.0 / math.pi)
GELU_K = 0.044715

N = 8192
D = 512
F = 2048
FB = 256
NB = F // FB
T1 = 512
N1 = N // T1
RH = T1 // 2
T2 = 2048
N2 = N // T2
RC2 = 128
RC1 = 256
KU2 = 512
KU1 = 256
RA = 128
TQ = T2 // T1
SLOTS = 4
SEMS = 8
OFFS = {2: (0, 2, 6, 10, 12, 16, 18), 1: (0, 1, 5, 8, 11, 15, 16)}
BASE = {2: 6, 1: 4 * (NB + 2) + 5}
LAST_TRIP = BASE[1] + 4 * (NB - 1) + OFFS[1][-1]

bf16 = jnp.bfloat16
f32 = jnp.float32


def dot(a, b):
    return jnp.dot(a, b, preferred_element_type=f32)


def gelu_half(a):
    sq = a * a
    t = jnp.tanh(a * (GELU_C + (GELU_C * GELU_K) * sq))
    s = 0.5 + 0.5 * t
    return sq, s, a * s


def gelu_and_grad(a):
    sq, s, h = gelu_half(a)
    g = s + (h * (1.0 - s)) * (2.0 * GELU_C + (6.0 * GELU_C * GELU_K) * sq)
    return h, g


def kernel(x_hbm, g_hbm, w1_hbm, w2_hbm, w3_hbm, w4_hbm, out, a1_hbm, da3_hbm,
           gn, gt, hn, ht, w1, w2, w3, w4, w4t, u0, u1, d0, d1, va, vb, xs,
           pacc, rx, sm, r1, r2, rs,
           ld_sem, x_sem, st_sem, ld2_sem, send_sem, recv_sem, loc_sem):
    z = lax.axis_index("z")
    y = lax.axis_index("y")
    c = lax.axis_index("xc")
    partner = (z, y, 1 - c)
    near_a = (lax.rem(z + c, 2), lax.rem(y + 1 - c, 2), c)
    near_b = (lax.rem(z + 1 - c, 2), lax.rem(y + c, 2), c)
    bit_a = y * (1 - c) + z * c
    bit_b = z * (1 - c) + y * c

    barrier = pltpu.get_barrier_semaphore()
    for dev in (partner, near_a, near_b):
        pl.semaphore_signal(barrier, inc=1, device_id=dev, device_id_type=MESH)

    def x_copy(i):
        slot = lax.rem(i, 4)
        return pltpu.make_async_copy(x_hbm.at[pl.ds(i * T1, T1)], xs.at[slot], x_sem.at[slot])

    loads = [
        pltpu.make_async_copy(w1_hbm, w1, ld_sem.at[0]),
        pltpu.make_async_copy(w2_hbm, w2, ld_sem.at[1]),
        pltpu.make_async_copy(g_hbm, gn, ld_sem.at[2]),
        pltpu.make_async_copy(w3_hbm, w3, ld_sem.at[3]),
        pltpu.make_async_copy(w4_hbm, w4, ld_sem.at[4]),
    ]
    loads[0].start()
    x_copy(0).start()
    x_copy(1).start()
    for ld in loads[1:]:
        ld.start()

    hs = (u0, u1)
    ds = (d0, d1)
    vs = (va, vb)

    def a1_store(i, par):
        return pltpu.make_async_copy(vs[par], a1_hbm.at[:, i], st_sem.at[par])

    def h1_tile(par, cc):
        return hs[cc // 4].at[cc % 4] if par == 0 else ds[cc // 4].at[cc % 4]

    def h2_unit(par, m, cc, total):
        term = dot(h1_tile(par, cc)[m * RH:(m + 1) * RH, :], w2[cc * FB:(cc + 1) * FB, :])
        return term if total is None else total + term

    def h2_store(i, m, total, x_rows):
        h2 = (total + x_rows.astype(f32)).astype(bf16)
        hn[pl.ds(pl.multiple_of(i * T1 + m * RH, RH), RH), :] = h2
        ht[i, :, m * RH:(m + 1) * RH] = h2.T

    def fwd_trip(i, par, with_a, with_b, with_gt=True):
        xt = xs.at[lax.rem(i, 4)]
        xp = xs.at[lax.rem(i + 3, 4)]
        total = None
        chunks = NB * (T1 // RA)
        for n in range(chunks):
            if with_a:
                cc, r = n // (T1 // RA), n % (T1 // RA)
                a = dot(xt[r * RA:(r + 1) * RA, :], w1[:, cc * FB:(cc + 1) * FB]).astype(bf16)
                vs[par][cc, r * RA:(r + 1) * RA, :] = a
                _, _, h = gelu_half(a.astype(f32))
                h1_tile(par, cc)[r * RA:(r + 1) * RA, :] = h.astype(bf16)
            if with_b:
                for n2 in range(n * 2 * NB // chunks, (n + 1) * 2 * NB // chunks):
                    m, cc = n2 // NB, n2 % NB
                    total = h2_unit(1 - par, m, cc, total if cc else None)
                    if cc == NB - 1:
                        h2_store(i - 1, m, total, xp[m * RH:(m + 1) * RH, :])
        if with_a and with_gt:
            rows = pl.ds(pl.multiple_of(i * T1, T1), T1)
            gt[i] = gn[rows, :].T

    def fwd_tail_transposes(i):
        lanes = pl.ds(pl.multiple_of(i * (F // N1), F // N1), F // N1)
        w4t[:, lanes] = w4[lanes, :].T

    loads[0].wait()
    x_copy(0).wait()
    x_copy(2).start()
    fwd_trip(0, 0, True, False, False)
    a1_store(0, 0).start()
    for ld in loads[1:]:
        ld.wait()
    gt[0] = gn[:T1, :].T
    fwd_tail_transposes(0)

    def fwd_pair(k, carry):
        for par in (1, 0):
            i = 2 * k + 2 - par

            @pl.when(i >= 2)
            def _():
                a1_store(i - 2, par).wait()

            @pl.when(i + 2 < N1)
            def _():
                x_copy(i + 2).start()

            x_copy(i).wait()
            fwd_trip(i, par, True, True)
            fwd_tail_transposes(i)
            a1_store(i, par).start()
        return carry

    lax.fori_loop(0, N1 // 2 - 1, fwd_pair, 0)
    a1_store(N1 - 3, 1).wait()
    x_copy(N1 - 1).wait()
    fwd_trip(N1 - 1, 1, True, True)
    fwd_tail_transposes(N1 - 1)
    a1_store(N1 - 1, 1).start()

    pl.semaphore_wait(barrier, 3)

    def half(b):
        return pl.ds(pl.multiple_of(b * (D // 2), D // 2), D // 2)

    def quarter(a, b):
        return pl.ds(pl.multiple_of(a * (D // 2) + b * (D // 4), D // 4), D // 4)

    def remote(src, dst, p, step, dev):
        e = lax.rem(p, SEMS)
        return pltpu.make_async_remote_copy(
            src_ref=src, dst_ref=dst, send_sem=send_sem.at[e, step], recv_sem=recv_sem.at[e, step],
            device_id=dev, device_id_type=MESH)

    def cp_pair(p):
        e = lax.rem(p, 2)
        return remote(pacc.at[e, 1 - c], rx.at[e], p, 0, partner)

    def cp_s1(p):
        e = lax.rem(p, 2)
        return remote(sm.at[e, half(1 - bit_a)], r1.at[e], p, 1, near_a)

    def cp_s2(p):
        e = lax.rem(p, 2)
        return remote(sm.at[e, quarter(bit_a, 1 - bit_b)], r2.at[e], p, 2, near_b)

    def cp_s3(p):
        part = rs.at[lax.rem(p, SLOTS), quarter(bit_a, bit_b)]
        return remote(part, part, p, 3, near_b)

    def cp_s4(p):
        part = rs.at[lax.rem(p, SLOTS), half(bit_a)]
        return remote(part, part, p, 4, near_a)

    def cp_s5(p):
        return remote(rs.at[lax.rem(p, SLOTS)], out.at[p, c], p, 5, partner)

    def cp_loc(p):
        e = lax.rem(p, SLOTS)
        return pltpu.make_async_copy(rs.at[e], out.at[p, c], loc_sem.at[e])

    def h_pair_send(p):
        cp_pair(p).start()

    def h_s1(p):
        cp_pair(p).wait()
        e = lax.rem(p, 2)
        sm[e] = pacc[e, c] + rx[e]
        cp_s1(p).start()

    def h_s2(p):
        cp_s1(p).wait()
        e = lax.rem(p, 2)
        rows = half(bit_a)
        sm[e, rows] = sm[e, rows] + r1[e]
        cp_s2(p).start()

    def h_s3(p):
        cp_s2(p).wait()
        e = lax.rem(p, 2)
        rows = quarter(bit_a, bit_b)
        rs[lax.rem(p, SLOTS), rows] = (sm[e, rows] + r2[e]) * 0.125
        cp_s3(p).start()

    def h_s4(p):
        cp_s3(p).wait()
        cp_s4(p).start()

    def h_s5(p):
        cp_s4(p).wait()
        cp_s5(p).start()
        cp_loc(p).start()

    def h_end(p):
        cp_s5(p).wait()
        cp_loc(p).wait()

    stages = (h_pair_send, h_s1, h_s2, h_s3, h_s4, h_s5, h_end)

    def comm(layer, f, parity):
        for order in (0, 6, 5, 4, 3, 2, 1):
            due = BASE[layer] + OFFS[layer][order]
            if (due - parity) % 2:
                continue
            q = f + (64 - due)
            k = q // 4 - 16

            @pl.when(jnp.logical_and(lax.rem(q, 4) == 0, jnp.logical_and(k >= 0, k < NB)))
            def _():
                stages[order](k if layer == 2 else k + NB)

    def b_unit(lhs0, lhs1, tb, par, rhs, first, ku, u, values):
        half_units = T2 // ku
        m, kq = u // half_units, u % half_units
        rows = slice(m * (D // 2), (m + 1) * (D // 2))
        lo = kq * ku
        out_values = []
        for idx, lhs in ((0, lhs0), (1, lhs1)):
            value = values[idx] if kq else None
            term = dot(lhs[tb * (T2 // T1) + lo // T1, rows, lo % T1:lo % T1 + ku], rhs[idx][lo // T1, lo % T1:lo % T1 + ku, :])
            value = term if value is None else value + term
            if kq == half_units - 1:
                old = pacc[par, idx, rows, :]
                if first is not None:
                    old = jnp.where(first, 0.0, old)
                pacc[par, idx, rows, :] = old + value
            out_values.append(value)
        return out_values

    def b_some(lhs0, lhs1, tb, par, rhs, first, ku, rc, chunks, values):
        units = 2 * (T2 // ku)
        for u in range(rc * units // chunks, (rc + 1) * units // chunks):
            values = b_unit(lhs0, lhs1, tb, par, rhs, first, ku, u, values)
        return values

    def b_part(lhs0, lhs1, tb, par, rhs, between=None):
        values = None
        for u in range(2 * (T2 // KU1)):
            values = b_unit(lhs0, lhs1, tb, par, rhs, None, KU1, u, values)
            if between is not None and u % 2 == 1:
                between(u // 2)

    def da3_store(f, par, e):
        return pltpu.make_async_copy(
            vs[par].at[pl.ds(e * TQ, TQ)], da3_hbm.at[f // N2, pl.ds(lax.rem(f, N2) * TQ, TQ)], st_sem.at[2 * e + par])

    def l2_trip(f, par, e, with_b=True):
        t = lax.rem(f, N2)
        j = f // N2
        col = pl.ds(pl.multiple_of(j * FB, FB), FB)
        before = f + N2 - 1
        tb = lax.rem(before, N2)
        pp = lax.rem(before // N2 + 1, 2)
        w3j = w3[:, col]
        w4j = w4t[:, col]
        rhs = (hs[1 - par], vb.at[pl.ds((1 - e) * TQ, TQ)] if par == 0 else va.at[pl.ds(e * TQ, TQ)])
        values = None
        first = None if par == 0 else tb == 0
        for rc in range(T2 // RC2):
            rows = pl.ds(pl.multiple_of(t * T2 + rc * RC2, RC2), RC2)
            tile, lo = rc * RC2 // T1, rc * RC2 % T1
            a = dot(hn[rows, :], w3j).astype(bf16).astype(f32)
            d = dot(gn[rows, :], w4j)
            h, g = gelu_and_grad(a)
            hs[par][tile, lo:lo + RC2, :] = h.astype(bf16)
            vs[par][e * TQ + tile, lo:lo + RC2, :] = (d * g).astype(bf16)
            if with_b:
                values = b_some(gt, ht, tb, pp, rhs, first, KU2, rc, T2 // RC2, values)
            else:
                values = last_h2(rc, values)

    def last_h2(rc, total):
        for n2 in range(rc * 2 * NB // (T2 // RC2), (rc + 1) * 2 * NB // (T2 // RC2)):
            m, cc = n2 // NB, n2 % NB
            total = h2_unit(1, m, cc, total if cc else None)
            if cc == NB - 1:
                h2_store(N1 - 1, m, total, xs[(N1 - 1) % 4, m * RH:(m + 1) * RH, :])
        return total

    for par in (0, 1):
        a1_store(N1 - 2 + par, par).wait()
    l2_trip(0, 0, 0, with_b=False)
    l2_trip(1, 1, 0)
    for par in (0, 1):
        da3_store(par, par, 0).start()

    def l2_pair(k, carry):
        e = lax.rem(k, 2)
        comm(2, 2 * k, 0)

        @pl.when(k >= 2)
        def _():
            for par in (0, 1):
                da3_store(2 * k - 4 + par, par, e).wait()

        for par in (0, 1):
            l2_trip(2 * k + par, par, e)
        for par in (0, 1):
            da3_store(2 * k + par, par, e).start()
        return carry

    lax.fori_loop(1, NB * N2 // 2, l2_pair, 0)

    tiles = ((va, vb), ((u0, u1), (d0, d1)))

    def da3_loads(i, e, par):
        tile = tiles[e][par]
        if e == 0:
            return [pltpu.make_async_copy(da3_hbm.at[:, i], tile, ld2_sem.at[par])]
        return [
            pltpu.make_async_copy(da3_hbm.at[pl.ds(h * TQ, TQ), i], tile[h], ld2_sem.at[2 + 2 * par + h])
            for h in (0, 1)]

    def da3_tile(e, par, cc):
        return tiles[0][par].at[cc] if e == 0 else tiles[1][par][cc // 4].at[cc % 4]

    def da3_start(i, e, par):
        for ld in da3_loads(i, e, par):
            ld.start()
        x_copy(i).start()

    def turn_weights(cc):
        cols = slice(cc * FB, (cc + 1) * FB)
        w4[cols, :] = w3[:, cols].T
        w4t[:, cols] = w2[cols, :].T

    for f0 in range(NB * N2 - 4, NB * N2):
        da3_store(f0, f0 % 2, f0 // 2 % 2).wait()
    da3_start(0, 0, 0)
    b_part(gt, ht, N2 - 1, (NB - 1) % 2, (hs[1], vb.at[pl.ds(TQ, TQ)]), turn_weights)
    da3_start(1, 0, 1)
    da3_start(2, 1, 0)
    da3_start(3, 1, 1)

    def dh2_tile(i, e, par):
        for m in (0, 1):
            rows = pl.ds(pl.multiple_of(i * T1 + m * RH, RH), RH)
            total = None
            for cc in range(NB):
                term = dot(da3_tile(e, par, cc)[m * RH:(m + 1) * RH, :], w4[cc * FB:(cc + 1) * FB, :])
                total = term if total is None else total + term
            dh2 = (total + gn[rows, :].astype(f32)).astype(bf16)
            hn[rows, :] = dh2
            ht[i, :, m * RH:(m + 1) * RH] = dh2.T
        gt[i] = xs[lax.rem(i, 4)].T

    def dh2_four(q, carry):
        comm(2, NB * N2 + 2 * q, 0)
        for e in (0, 1):
            for par in (0, 1):
                i = 4 * q + 2 * e + par
                for ld in da3_loads(i, e, par):
                    ld.wait()
                x_copy(i).wait()
            for par in (0, 1):
                dh2_tile(4 * q + 2 * e + par, e, par)

            @pl.when(q < N1 // 4 - 1)
            def _():
                for par in (0, 1):
                    da3_start(4 * q + 4 + 2 * e + par, e, par)
        return carry

    lax.fori_loop(0, N1 // 4, dh2_four, 0)

    base = NB * N2 + N1 // 2

    def a1_load(k, par):
        f = 2 * k + par
        e = lax.rem(k, 2)
        return pltpu.make_async_copy(
            a1_hbm.at[f // N2, pl.ds(lax.rem(f, N2) * TQ, TQ)], vs[par].at[pl.ds(e * TQ, TQ)], x_sem.at[2 * e + par])

    for par in (0, 1):
        a1_load(0, par).start()

    def l1_trip(f, par):
        t = lax.rem(f, N2)
        j = f // N2
        col = pl.ds(pl.multiple_of(j * FB, FB), FB)
        before = f + N2 - 1
        tb = lax.rem(before, N2)
        pp = lax.rem(before // N2 + 1, 2)
        e = lax.rem(f // 2, 2)
        w2j = w4t[:, col]
        rhs = (hs[1 - par], ds[1 - par])
        values = None
        for rc in range(T2 // RC1):
            rows = pl.ds(pl.multiple_of(t * T2 + rc * RC1, RC1), RC1)
            tile, lo = rc * RC1 // T1, rc * RC1 % T1
            a = vs[par][e * TQ + tile, lo:lo + RC1, :].astype(f32)
            d = dot(hn[rows, :], w2j)
            h, g = gelu_and_grad(a)
            hs[par][tile, lo:lo + RC1, :] = h.astype(bf16)
            ds[par][tile, lo:lo + RC1, :] = (d * g).astype(bf16)
            values = b_some(ht, gt, tb, pp, rhs, None if par == 0 else tb == 0, KU1, rc, T2 // RC1, values)

    def l1_pair(k, carry):
        for par in (0, 1):
            f = base + 2 * k + par
            comm(2, f, par)
            comm(1, f, par)
            a1_load(k, par).wait()

            @pl.when(2 * k + 2 < NB * N2)
            def _():
                a1_load(k + 1, par).start()

            l1_trip(2 * k + par, par)
        return carry

    lax.fori_loop(0, NB * N2 // 2, l1_pair, 0)
    comm(1, base + NB * N2, 0)
    b_part(ht, gt, N2 - 1, (NB - 1) % 2, (hs[1], ds[1]))

    def tail(k, carry):
        for par in (1, 0):
            comm(1, base + NB * N2 + 2 + 2 * k - par, par)
        return carry

    lax.fori_loop(0, (LAST_TRIP - base - NB * N2 + 1) // 2, tail, 0)


def finish_kernel(sums, o1, o2, o3, o4, buf, flip, in_sem, wide_sem, tall_sem):
    def load(p):
        return pltpu.make_async_copy(sums.at[p], buf.at[p], in_sem.at[p])

    def store_wide(o, j, p):
        return pltpu.make_async_copy(
            buf.at[p, 1], o.at[:, pl.ds(pl.multiple_of(j * FB, FB), FB)], wide_sem.at[p])

    def store_tall(o, j, p):
        return pltpu.make_async_copy(
            flip.at[p], o.at[pl.ds(pl.multiple_of(j * FB, FB), FB), :], tall_sem.at[p])

    for p in range(2 * NB):
        load(p).start()
    for base, wide, tall in ((0, o3, o4), (NB, o1, o2)):
        def step(j, carry):
            p = base + j
            load(p).wait()
            store_wide(wide, j, p).start()
            flip[p] = buf[p, 0].T
            store_tall(tall, j, p).start()
            return carry
        lax.fori_loop(0, NB, step, 0)
    for base, wide, tall in ((0, o3, o4), (NB, o1, o2)):
        def drain(j, carry):
            store_wide(wide, j, base + j).wait()
            store_tall(tall, j, base + j).wait()
            return carry
        lax.fori_loop(0, NB, drain, 0)


def device_step(x_loc, g_loc, w_one, w_two, w_three, w_four):
    any_spec = pl.BlockSpec(memory_space=pl.ANY)
    sums, _, _ = pl.pallas_call(
        kernel,
        name="grads",
        out_shape=(
            jax.ShapeDtypeStruct((2 * NB, 2, D, FB), f32),
            jax.ShapeDtypeStruct((NB, N1, T1, FB), bf16),
            jax.ShapeDtypeStruct((NB, N1, T1, FB), bf16),
        ),
        in_specs=[any_spec] * 6,
        out_specs=(any_spec,) * 3,
        scratch_shapes=[
            pltpu.VMEM((N, D), bf16),
            pltpu.VMEM((N1, D, T1), bf16),
            pltpu.VMEM((N, D), bf16),
            pltpu.VMEM((N1, D, T1), bf16),
            pltpu.VMEM((D, F), bf16),
            pltpu.VMEM((F, D), bf16),
            pltpu.VMEM((D, F), bf16),
            pltpu.VMEM((F, D), bf16),
            pltpu.VMEM((D, F), bf16),
            pltpu.VMEM((TQ, T1, FB), bf16),
            pltpu.VMEM((TQ, T1, FB), bf16),
            pltpu.VMEM((TQ, T1, FB), bf16),
            pltpu.VMEM((TQ, T1, FB), bf16),
            pltpu.VMEM((NB, T1, FB), bf16),
            pltpu.VMEM((NB, T1, FB), bf16),
            pltpu.VMEM((4, T1, D), bf16),
            pltpu.VMEM((2, 2, D, FB), f32),
            pltpu.VMEM((2, D, FB), f32),
            pltpu.VMEM((2, D, FB), f32),
            pltpu.VMEM((2, D // 2, FB), f32),
            pltpu.VMEM((2, D // 4, FB), f32),
            pltpu.VMEM((SLOTS, D, FB), f32),
            pltpu.SemaphoreType.DMA((5,)),
            pltpu.SemaphoreType.DMA((4,)),
            pltpu.SemaphoreType.DMA((4,)),
            pltpu.SemaphoreType.DMA((6,)),
            pltpu.SemaphoreType.DMA((SEMS, 6)),
            pltpu.SemaphoreType.DMA((SEMS, 6)),
            pltpu.SemaphoreType.DMA((SLOTS,)),
        ],
        compiler_params=pltpu.CompilerParams(
            collective_id=0, has_side_effects=True, vmem_limit_bytes=67000000),
        cost_estimate=pl.CostEstimate(flops=20 * N * D * F, bytes_accessed=200 << 20, transcendentals=3 * N * F),
    )(x_loc, g_loc, w_one, w_two, w_three, w_four)
    wide = jax.ShapeDtypeStruct((D, F), f32)
    tall = jax.ShapeDtypeStruct((F, D), f32)
    return pl.pallas_call(
        finish_kernel,
        name="finish",
        out_shape=(wide, tall, wide, tall),
        in_specs=[any_spec],
        out_specs=(any_spec,) * 4,
        scratch_shapes=[
            pltpu.VMEM((2 * NB, 2, D, FB), f32),
            pltpu.VMEM((2 * NB, FB, D), f32),
            pltpu.SemaphoreType.DMA((2 * NB,)),
            pltpu.SemaphoreType.DMA((2 * NB,)),
            pltpu.SemaphoreType.DMA((2 * NB,)),
        ],
        compiler_params=pltpu.CompilerParams(vmem_limit_bytes=40 << 20),
    )(sums)


def solution(mesh):
    batch_spec = P(("z", "y", "xc"), None)
    whole_spec = P(None, None)
    return jax.shard_map(
        device_step,
        mesh=mesh,
        in_specs=(batch_spec, batch_spec, whole_spec, whole_spec, whole_spec, whole_spec),
        out_specs=(whole_spec, whole_spec, whole_spec, whole_spec),
        check_vma=False,
    )
```

```python
import functools
import math

import jax
import jax.numpy as jnp
from jax import lax
from jax.experimental import pallas as pl
from jax.experimental.pallas import tpu as pltpu
from jax.sharding import PartitionSpec as P

MESH = pl.DeviceIdType.MESH
GELU_C = math.sqrt(2.0 / math.pi)
GELU_K = 0.044715

N = 8192
D = 512
F = 2048
FB = 256
NB = F // FB
T1 = 512
N1 = N // T1
RH = T1 // 2
T2 = 2048
N2 = N // T2
RC2 = 128
RC1 = 256
KU2 = 512
KU1 = 256
RA = 128
TQ = T2 // T1
SLOTS = 4
SEMS = 8
OFFS = {2: (0, 2, 6, 10, 12, 16, 18), 1: (0, 1, 5, 8, 11, 15, 16)}
BASE = {2: 6, 1: 4 * (NB + 2) + 5}
LAST_TRIP = BASE[1] + 4 * (NB - 1) + OFFS[1][-1]

bf16 = jnp.bfloat16
f32 = jnp.float32


def dot(a, b):
    return jnp.dot(a, b, preferred_element_type=f32)


def gelu_half(a):
    sq = a * a
    t = jnp.tanh(a * (GELU_C + (GELU_C * GELU_K) * sq))
    s = 0.5 + 0.5 * t
    return sq, s, a * s


def gelu_and_grad(a):
    sq, s, h = gelu_half(a)
    g = s + (h * (1.0 - s)) * (2.0 * GELU_C + (6.0 * GELU_C * GELU_K) * sq)
    return h, g


def kernel(x_hbm, g_hbm, w1_hbm, w2_hbm, w3_hbm, w4_hbm, out, a1_hbm, da3_hbm,
           gn, gt, hn, ht, w1, w2, w3, w4, w4t, u0, u1, d0, d1, va, vb, xs,
           pacc, rx, sm, r1, r2, rs,
           ld_sem, x_sem, st_sem, ld2_sem, send_sem, recv_sem, loc_sem):
    z = lax.axis_index("z")
    y = lax.axis_index("y")
    c = lax.axis_index("xc")
    partner = (z, y, 1 - c)
    near_a = (lax.rem(z + c, 2), lax.rem(y + 1 - c, 2), c)
    near_b = (lax.rem(z + 1 - c, 2), lax.rem(y + c, 2), c)
    bit_a = y * (1 - c) + z * c
    bit_b = z * (1 - c) + y * c

    barrier = pltpu.get_barrier_semaphore()
    for dev in (partner, near_a, near_b):
        pl.semaphore_signal(barrier, inc=1, device_id=dev, device_id_type=MESH)

    def x_copy(i):
        slot = lax.rem(i, 4)
        return pltpu.make_async_copy(x_hbm.at[pl.ds(i * T1, T1)], xs.at[slot], x_sem.at[slot])

    g_head, g_rest = pl.ds(0, N // 2), pl.ds(N // 2, N // 2)
    loads = [
        pltpu.make_async_copy(w1_hbm, w1, ld_sem.at[0]),
        pltpu.make_async_copy(w2_hbm, w2, ld_sem.at[1]),
        pltpu.make_async_copy(g_hbm.at[g_head], gn.at[g_head], ld_sem.at[2]),
        pltpu.make_async_copy(w4_hbm, w4, ld_sem.at[3]),
        pltpu.make_async_copy(g_hbm.at[g_rest], gn.at[g_rest], ld_sem.at[4]),
        pltpu.make_async_copy(w3_hbm, w3, ld_sem.at[5]),
    ]
    loads[0].start()
    x_copy(0).start()

    hs = (u0, u1)
    ds = (d0, d1)
    vs = (va, vb)

    def a1_store(i, par):
        return pltpu.make_async_copy(vs[par], a1_hbm.at[:, i], st_sem.at[par])

    def h1_tile(par, cc):
        return hs[cc // 4].at[cc % 4] if par == 0 else ds[cc // 4].at[cc % 4]

    def h2_unit(par, m, cc, total):
        term = dot(h1_tile(par, cc)[m * RH:(m + 1) * RH, :], w2[cc * FB:(cc + 1) * FB, :])
        return term if total is None else total + term

    def h2_store(i, m, total, x_rows):
        h2 = (total + x_rows.astype(f32)).astype(bf16)
        hn[pl.ds(pl.multiple_of(i * T1 + m * RH, RH), RH), :] = h2
        ht[i, :, m * RH:(m + 1) * RH] = h2.T

    def fwd_trip(i, par, with_a, with_b, with_gt=True):
        xt = xs.at[lax.rem(i, 4)]
        xp = xs.at[lax.rem(i + 3, 4)]
        total = None
        chunks = NB * (T1 // RA)
        for n in range(chunks):
            if with_a:
                cc, r = n // (T1 // RA), n % (T1 // RA)
                a = dot(xt[r * RA:(r + 1) * RA, :], w1[:, cc * FB:(cc + 1) * FB]).astype(bf16)
                vs[par][cc, r * RA:(r + 1) * RA, :] = a
                _, _, h = gelu_half(a.astype(f32))
                h1_tile(par, cc)[r * RA:(r + 1) * RA, :] = h.astype(bf16)
            if with_b:
                for n2 in range(n * 2 * NB // chunks, (n + 1) * 2 * NB // chunks):
                    m, cc = n2 // NB, n2 % NB
                    total = h2_unit(1 - par, m, cc, total if cc else None)
                    if cc == NB - 1:
                        h2_store(i - 1, m, total, xp[m * RH:(m + 1) * RH, :])
        if with_a and with_gt:
            rows = pl.ds(pl.multiple_of(i * T1, T1), T1)
            gt[i] = gn[rows, :].T

    def fwd_tail_transposes(i):
        lanes = pl.ds(pl.multiple_of(i * (F // N1), F // N1), F // N1)
        w4t[:, lanes] = w4[lanes, :].T

    loads[0].wait()
    x_copy(0).wait()
    x_copy(1).start()
    for ld in loads[1:]:
        ld.start()
    x_copy(2).start()
    fwd_trip(0, 0, True, False, False)
    a1_store(0, 0).start()
    for ld in loads[1:4]:
        ld.wait()
    gt[0] = gn[:T1, :].T
    fwd_tail_transposes(0)

    def fwd_pair(k, carry):
        @pl.when(k == 2)
        def _():
            for ld in loads[4:]:
                ld.wait()

        for par in (1, 0):
            i = 2 * k + 2 - par

            @pl.when(i >= 2)
            def _():
                a1_store(i - 2, par).wait()

            @pl.when(i + 2 < N1)
            def _():
                x_copy(i + 2).start()

            x_copy(i).wait()
            fwd_trip(i, par, True, True)
            fwd_tail_transposes(i)
            a1_store(i, par).start()
        return carry

    lax.fori_loop(0, N1 // 2 - 1, fwd_pair, 0)
    a1_store(N1 - 3, 1).wait()
    x_copy(N1 - 1).wait()
    fwd_trip(N1 - 1, 1, True, True)
    fwd_tail_transposes(N1 - 1)
    a1_store(N1 - 1, 1).start()

    pl.semaphore_wait(barrier, 3)

    def half(b):
        return pl.ds(pl.multiple_of(b * (D // 2), D // 2), D // 2)

    def quarter(a, b):
        return pl.ds(pl.multiple_of(a * (D // 2) + b * (D // 4), D // 4), D // 4)

    def remote(src, dst, p, step, dev):
        e = lax.rem(p, SEMS)
        return pltpu.make_async_remote_copy(
            src_ref=src, dst_ref=dst, send_sem=send_sem.at[e, step], recv_sem=recv_sem.at[e, step],
            device_id=dev, device_id_type=MESH)

    def cp_pair(p):
        e = lax.rem(p, 2)
        return remote(pacc.at[e, 1 - c], rx.at[e], p, 0, partner)

    def cp_s1(p):
        e = lax.rem(p, 2)
        return remote(sm.at[e, half(1 - bit_a)], r1.at[e], p, 1, near_a)

    def cp_s2(p):
        e = lax.rem(p, 2)
        return remote(sm.at[e, quarter(bit_a, 1 - bit_b)], r2.at[e], p, 2, near_b)

    def cp_s3(p):
        part = rs.at[lax.rem(p, SLOTS), quarter(bit_a, bit_b)]
        return remote(part, part, p, 3, near_b)

    def cp_s4(p):
        part = rs.at[lax.rem(p, SLOTS), half(bit_a)]
        return remote(part, part, p, 4, near_a)

    def cp_s5(p):
        return remote(rs.at[lax.rem(p, SLOTS)], out.at[p, c], p, 5, partner)

    def cp_loc(p):
        e = lax.rem(p, SLOTS)
        return pltpu.make_async_copy(rs.at[e], out.at[p, c], loc_sem.at[e])

    def h_pair_send(p):
        cp_pair(p).start()

    def h_s1(p):
        cp_pair(p).wait()
        e = lax.rem(p, 2)
        sm[e] = pacc[e, c] + rx[e]
        cp_s1(p).start()

    def h_s2(p):
        cp_s1(p).wait()
        e = lax.rem(p, 2)
        rows = half(bit_a)
        sm[e, rows] = sm[e, rows] + r1[e]
        cp_s2(p).start()

    def h_s3(p):
        cp_s2(p).wait()
        e = lax.rem(p, 2)
        rows = quarter(bit_a, bit_b)
        rs[lax.rem(p, SLOTS), rows] = (sm[e, rows] + r2[e]) * 0.125
        cp_s3(p).start()

    def h_s4(p):
        cp_s3(p).wait()
        cp_s4(p).start()

    def h_s5(p):
        cp_s4(p).wait()
        cp_s5(p).start()
        cp_loc(p).start()

    def h_end(p):
        cp_s5(p).wait()
        cp_loc(p).wait()

    stages = (h_pair_send, h_s1, h_s2, h_s3, h_s4, h_s5, h_end)

    def comm(layer, f, parity):
        for order in (0, 6, 5, 4, 3, 2, 1):
            due = BASE[layer] + OFFS[layer][order]
            if (due - parity) % 2:
                continue
            q = f + (64 - due)
            k = q // 4 - 16

            @pl.when(jnp.logical_and(lax.rem(q, 4) == 0, jnp.logical_and(k >= 0, k < NB)))
            def _():
                stages[order](k if layer == 2 else k + NB)

    def b_unit(lhs0, lhs1, tb, par, rhs, first, ku, u, values):
        half_units = T2 // ku
        m, kq = u // half_units, u % half_units
        rows = slice(m * (D // 2), (m + 1) * (D // 2))
        lo = kq * ku
        out_values = []
        for idx, lhs in ((0, lhs0), (1, lhs1)):
            value = values[idx] if kq else None
            term = dot(lhs[tb * (T2 // T1) + lo // T1, rows, lo % T1:lo % T1 + ku], rhs[idx][lo // T1, lo % T1:lo % T1 + ku, :])
            value = term if value is None else value + term
            if kq == half_units - 1:
                old = pacc[par, idx, rows, :]
                if first is not None:
                    old = jnp.where(first, 0.0, old)
                pacc[par, idx, rows, :] = old + value
            out_values.append(value)
        return out_values

    def b_some(lhs0, lhs1, tb, par, rhs, first, ku, rc, chunks, values):
        units = 2 * (T2 // ku)
        for u in range(rc * units // chunks, (rc + 1) * units // chunks):
            values = b_unit(lhs0, lhs1, tb, par, rhs, first, ku, u, values)
        return values

    def b_part(lhs0, lhs1, tb, par, rhs, between=None):
        values = None
        for u in range(2 * (T2 // KU1)):
            values = b_unit(lhs0, lhs1, tb, par, rhs, None, KU1, u, values)
            if between is not None and u % 2 == 1:
                between(u // 2)

    def da3_store(f, par, e):
        return pltpu.make_async_copy(
            vs[par].at[pl.ds(e * TQ, TQ)], da3_hbm.at[f // N2, pl.ds(lax.rem(f, N2) * TQ, TQ)], st_sem.at[2 * e + par])

    def l2_trip(f, par, e, with_b=True):
        t = lax.rem(f, N2)
        j = f // N2
        col = pl.ds(pl.multiple_of(j * FB, FB), FB)
        before = f + N2 - 1
        tb = lax.rem(before, N2)
        pp = lax.rem(before // N2 + 1, 2)
        w3j = w3[:, col]
        w4j = w4t[:, col]
        rhs = (hs[1 - par], vb.at[pl.ds((1 - e) * TQ, TQ)] if par == 0 else va.at[pl.ds(e * TQ, TQ)])
        values = None
        first = None if par == 0 else tb == 0
        for rc in range(T2 // RC2):
            rows = pl.ds(pl.multiple_of(t * T2 + rc * RC2, RC2), RC2)
            tile, lo = rc * RC2 // T1, rc * RC2 % T1
            a = dot(hn[rows, :], w3j).astype(bf16).astype(f32)
            d = dot(gn[rows, :], w4j)
            h, g = gelu_and_grad(a)
            hs[par][tile, lo:lo + RC2, :] = h.astype(bf16)
            vs[par][e * TQ + tile, lo:lo + RC2, :] = (d * g).astype(bf16)
            if with_b:
                values = b_some(gt, ht, tb, pp, rhs, first, KU2, rc, T2 // RC2, values)
            else:
                values = last_h2(rc, values)

    def last_h2(rc, total):
        for n2 in range(rc * 2 * NB // (T2 // RC2), (rc + 1) * 2 * NB // (T2 // RC2)):
            m, cc = n2 // NB, n2 % NB
            total = h2_unit(1, m, cc, total if cc else None)
            if cc == NB - 1:
                h2_store(N1 - 1, m, total, xs[(N1 - 1) % 4, m * RH:(m + 1) * RH, :])
        return total

    for par in (0, 1):
        a1_store(N1 - 2 + par, par).wait()
    l2_trip(0, 0, 0, with_b=False)
    l2_trip(1, 1, 0)
    for par in (0, 1):
        da3_store(par, par, 0).start()

    def l2_pair(k, carry):
        e = lax.rem(k, 2)
        comm(2, 2 * k, 0)

        @pl.when(k >= 2)
        def _():
            for par in (0, 1):
                da3_store(2 * k - 4 + par, par, e).wait()

        for par in (0, 1):
            l2_trip(2 * k + par, par, e)
        for par in (0, 1):
            da3_store(2 * k + par, par, e).start()
        return carry

    lax.fori_loop(1, NB * N2 // 2, l2_pair, 0)

    tiles = ((va, vb), ((u0, u1), (d0, d1)))

    def da3_loads(i, e, par):
        tile = tiles[e][par]
        if e == 0:
            return [pltpu.make_async_copy(da3_hbm.at[:, i], tile, ld2_sem.at[par])]
        return [
            pltpu.make_async_copy(da3_hbm.at[pl.ds(h * TQ, TQ), i], tile[h], ld2_sem.at[2 + 2 * par + h])
            for h in (0, 1)]

    def da3_tile(e, par, cc):
        return tiles[0][par].at[cc] if e == 0 else tiles[1][par][cc // 4].at[cc % 4]

    def da3_start(i, e, par):
        for ld in da3_loads(i, e, par):
            ld.start()
        x_copy(i).start()

    def turn_weights(cc):
        cols = slice(cc * FB, (cc + 1) * FB)
        w4[cols, :] = w3[:, cols].T
        w4t[:, cols] = w2[cols, :].T

    for f0 in range(NB * N2 - 4, NB * N2):
        da3_store(f0, f0 % 2, f0 // 2 % 2).wait()
    da3_start(0, 0, 0)
    b_part(gt, ht, N2 - 1, (NB - 1) % 2, (hs[1], vb.at[pl.ds(TQ, TQ)]), turn_weights)
    da3_start(1, 0, 1)
    da3_start(2, 1, 0)
    da3_start(3, 1, 1)

    def dh2_tile(i, e, par):
        for m in (0, 1):
            rows = pl.ds(pl.multiple_of(i * T1 + m * RH, RH), RH)
            total = None
            for cc in range(NB):
                term = dot(da3_tile(e, par, cc)[m * RH:(m + 1) * RH, :], w4[cc * FB:(cc + 1) * FB, :])
                total = term if total is None else total + term
            dh2 = (total + gn[rows, :].astype(f32)).astype(bf16)
            hn[rows, :] = dh2
            ht[i, :, m * RH:(m + 1) * RH] = dh2.T
        gt[i] = xs[lax.rem(i, 4)].T

    def dh2_four(q, carry):
        comm(2, NB * N2 + 2 * q, 0)
        for e in (0, 1):
            for par in (0, 1):
                i = 4 * q + 2 * e + par
                for ld in da3_loads(i, e, par):
                    ld.wait()
                x_copy(i).wait()
            for par in (0, 1):
                dh2_tile(4 * q + 2 * e + par, e, par)

            @pl.when(q < N1 // 4 - 1)
            def _():
                for par in (0, 1):
                    da3_start(4 * q + 4 + 2 * e + par, e, par)
        return carry

    lax.fori_loop(0, N1 // 4, dh2_four, 0)

    base = NB * N2 + N1 // 2

    def a1_load(k, par):
        f = 2 * k + par
        e = lax.rem(k, 2)
        return pltpu.make_async_copy(
            a1_hbm.at[f // N2, pl.ds(lax.rem(f, N2) * TQ, TQ)], vs[par].at[pl.ds(e * TQ, TQ)], x_sem.at[2 * e + par])

    for par in (0, 1):
        a1_load(0, par).start()

    def l1_trip(f, par):
        t = lax.rem(f, N2)
        j = f // N2
        col = pl.ds(pl.multiple_of(j * FB, FB), FB)
        before = f + N2 - 1
        tb = lax.rem(before, N2)
        pp = lax.rem(before // N2 + 1, 2)
        e = lax.rem(f // 2, 2)
        w2j = w4t[:, col]
        rhs = (hs[1 - par], ds[1 - par])
        values = None
        for rc in range(T2 // RC1):
            rows = pl.ds(pl.multiple_of(t * T2 + rc * RC1, RC1), RC1)
            tile, lo = rc * RC1 // T1, rc * RC1 % T1
            a = vs[par][e * TQ + tile, lo:lo + RC1, :].astype(f32)
            d = dot(hn[rows, :], w2j)
            h, g = gelu_and_grad(a)
            hs[par][tile, lo:lo + RC1, :] = h.astype(bf16)
            ds[par][tile, lo:lo + RC1, :] = (d * g).astype(bf16)
            values = b_some(ht, gt, tb, pp, rhs, None if par == 0 else tb == 0, KU1, rc, T2 // RC1, values)

    def l1_pair(k, carry):
        for par in (0, 1):
            f = base + 2 * k + par
            comm(2, f, par)
            comm(1, f, par)
            a1_load(k, par).wait()

            @pl.when(2 * k + 2 < NB * N2)
            def _():
                a1_load(k + 1, par).start()

            l1_trip(2 * k + par, par)
        return carry

    lax.fori_loop(0, NB * N2 // 2, l1_pair, 0)
    comm(1, base + NB * N2, 0)
    b_part(ht, gt, N2 - 1, (NB - 1) % 2, (hs[1], ds[1]))

    def tail(k, carry):
        for par in (1, 0):
            comm(1, base + NB * N2 + 2 + 2 * k - par, par)
        return carry

    lax.fori_loop(0, (LAST_TRIP - base - NB * N2 + 1) // 2, tail, 0)


def finish_kernel(sums, o1, o2, o3, o4, buf, flip, in_sem, wide_sem, tall_sem):
    def load(p):
        return pltpu.make_async_copy(sums.at[p], buf.at[p], in_sem.at[p])

    def store_wide(o, j, p):
        return pltpu.make_async_copy(
            buf.at[p, 1], o.at[:, pl.ds(pl.multiple_of(j * FB, FB), FB)], wide_sem.at[p])

    def store_tall(o, j, p):
        return pltpu.make_async_copy(
            flip.at[p], o.at[pl.ds(pl.multiple_of(j * FB, FB), FB), :], tall_sem.at[p])

    for p in range(2 * NB):
        load(p).start()
    for base, wide, tall in ((0, o3, o4), (NB, o1, o2)):
        def step(j, carry):
            p = base + j
            load(p).wait()
            store_wide(wide, j, p).start()
            flip[p] = buf[p, 0].T
            store_tall(tall, j, p).start()
            return carry
        lax.fori_loop(0, NB, step, 0)
    for base, wide, tall in ((0, o3, o4), (NB, o1, o2)):
        def drain(j, carry):
            store_wide(wide, j, base + j).wait()
            store_tall(tall, j, base + j).wait()
            return carry
        lax.fori_loop(0, NB, drain, 0)


def device_step(x_loc, g_loc, w_one, w_two, w_three, w_four):
    any_spec = pl.BlockSpec(memory_space=pl.ANY)
    sums, _, _ = pl.pallas_call(
        kernel,
        name="grads",
        out_shape=(
            jax.ShapeDtypeStruct((2 * NB, 2, D, FB), f32),
            jax.ShapeDtypeStruct((NB, N1, T1, FB), bf16),
            jax.ShapeDtypeStruct((NB, N1, T1, FB), bf16),
        ),
        in_specs=[any_spec] * 6,
        out_specs=(any_spec,) * 3,
        scratch_shapes=[
            pltpu.VMEM((N, D), bf16),
            pltpu.VMEM((N1, D, T1), bf16),
            pltpu.VMEM((N, D), bf16),
            pltpu.VMEM((N1, D, T1), bf16),
            pltpu.VMEM((D, F), bf16),
            pltpu.VMEM((F, D), bf16),
            pltpu.VMEM((D, F), bf16),
            pltpu.VMEM((F, D), bf16),
            pltpu.VMEM((D, F), bf16),
            pltpu.VMEM((TQ, T1, FB), bf16),
            pltpu.VMEM((TQ, T1, FB), bf16),
            pltpu.VMEM((TQ, T1, FB), bf16),
            pltpu.VMEM((TQ, T1, FB), bf16),
            pltpu.VMEM((NB, T1, FB), bf16),
            pltpu.VMEM((NB, T1, FB), bf16),
            pltpu.VMEM((4, T1, D), bf16),
            pltpu.VMEM((2, 2, D, FB), f32),
            pltpu.VMEM((2, D, FB), f32),
            pltpu.VMEM((2, D, FB), f32),
            pltpu.VMEM((2, D // 2, FB), f32),
            pltpu.VMEM((2, D // 4, FB), f32),
            pltpu.VMEM((SLOTS, D, FB), f32),
            pltpu.SemaphoreType.DMA((6,)),
            pltpu.SemaphoreType.DMA((4,)),
            pltpu.SemaphoreType.DMA((4,)),
            pltpu.SemaphoreType.DMA((6,)),
            pltpu.SemaphoreType.DMA((SEMS, 6)),
            pltpu.SemaphoreType.DMA((SEMS, 6)),
            pltpu.SemaphoreType.DMA((SLOTS,)),
        ],
        compiler_params=pltpu.CompilerParams(
            collective_id=0, has_side_effects=True, vmem_limit_bytes=67000000),
        cost_estimate=pl.CostEstimate(flops=20 * N * D * F, bytes_accessed=200 << 20, transcendentals=3 * N * F),
    )(x_loc, g_loc, w_one, w_two, w_three, w_four)
    wide = jax.ShapeDtypeStruct((D, F), f32)
    tall = jax.ShapeDtypeStruct((F, D), f32)
    return pl.pallas_call(
        finish_kernel,
        name="finish",
        out_shape=(wide, tall, wide, tall),
        in_specs=[any_spec],
        out_specs=(any_spec,) * 4,
        scratch_shapes=[
            pltpu.VMEM((2 * NB, 2, D, FB), f32),
            pltpu.VMEM((2 * NB, FB, D), f32),
            pltpu.SemaphoreType.DMA((2 * NB,)),
            pltpu.SemaphoreType.DMA((2 * NB,)),
            pltpu.SemaphoreType.DMA((2 * NB,)),
        ],
        compiler_params=pltpu.CompilerParams(vmem_limit_bytes=40 << 20),
    )(sums)


def solution(mesh):
    batch_spec = P(("z", "y", "xc"), None)
    whole_spec = P(None, None)
    return jax.shard_map(
        device_step,
        mesh=mesh,
        in_specs=(batch_spec, batch_spec, whole_spec, whole_spec, whole_spec, whole_spec),
        out_specs=(whole_spec, whole_spec, whole_spec, whole_spec),
        check_vma=False,
    )
```
